32 devices in a mesh: parts: 2 (over x), cluster: 16 (over z, y, core).
Axes of the slice: x: 2, y: 2, z: 4, core: 2. Of those that a mesh axis runs over, the one named last changes fastest.
Arguments:
- queries: float32 [4096, 1024], P(('parts', 'cluster')), parts along dimension 0, may hold values from -1 to 1
- passages: float32 [64, 128, 1024], P(('parts', 'cluster')), parts along dimension 0, may hold values from -6 to 6
- first_blocks: int32 [4096, 4], P(('parts', 'cluster')), parts along dimension 0, may hold values from 0 to 31, all different within a row; in each aligned block of 128 rows (0 to 127, 128 to 255, ...) at most 24 rows name the same one
- followup_blocks: int32 [4096, 4], P(('parts', 'cluster')), parts along dimension 0, may hold values from 0 to 31, all different within a row; in each aligned block of 128 rows (0 to 127, 128 to 255, ...) at most 24 rows name the same one
Outputs:
- expanded: float32 [4096, 1024], P(('parts', 'cluster')), parts along dimension 0
- second_scores: float32 [4096, 4, 128], P(('parts', 'cluster')), parts along dimension 0
The draws below stay inside these ranges and needn't reach their ends.
There are 2 independent parts, one for each index of `parts`. The reference program is written for one: setup_inputs(seed, part) draws one part's arguments, and reference() takes and returns one part's arrays. A program takes and returns all parts, laid end to end along the dimension named above; each array names one. Nothing has to cross between parts.
Inputs may be any that keep to these rules, and one draw needn't show every extreme that they name: `first_blocks`: each row names 4 different blocks; among the queries of one device no block is named more than 24 times, and some block is named exactly 24 times. `followup_blocks`: each row names 4 different blocks; among the queries of one device no block is named more than 24 times, and some block is named exactly 24 times.
All inputs are finite; a program needn't handle non-finite values.
Results may differ from the reference program's by a relative error of at most 0.00014.
Values sent between devices are 32-bit elements; how exact they have to be, the bound alone decides.
A program may use at most 128 MiB of HBM per device.

```python
import math
from functools import partial
import jax
import jax.numpy as jnp
import numpy as np
from jax import lax

E = 1024
ROWS = 128
KB = 4
Q_DEV = 128
NBLK = 32
QUERIES = 2048
CAP = 24


def draw_queries(key, part):
    bound = float((E + 160) // E)
    base = jax.random.normal(jax.random.fold_in(key, 7002), (QUERIES, E), jnp.float32) * E ** (-0.5)
    return jnp.clip(base, -bound, bound)


def draw_passages(key, part):
    noise = jax.random.normal(jax.random.fold_in(key, 7005), (NBLK, ROWS, E), jnp.float32)
    values = noise
    return jnp.clip(values, -6.0, 6.0)


def shared_out(own_key, own, number, rows, count, top, most, slope):
    order = jax.random.permutation(own_key, count)
    crowded, usual = shares(count, rows * top, most, slope, True), shares(count, rows * top, most, slope, False)
    places = jnp.arange(count)

    def named(sizes, offset_by):
        used = int((sizes > 0).sum())
        fixed = max(1, used // 4)
        moved = fixed + (places - fixed + offset_by * (used - fixed)) % max(1, count - fixed)
        return jnp.zeros((count,), jnp.int32).at[order[jnp.where(places < fixed, places, moved)]].set(jnp.asarray(sizes, jnp.int32))

    sizes = jnp.where(number % 4 == 0, named(crowded, number // 4), named(usual, number - number // 4 - 1))
    mixed = jax.random.permutation(jax.random.fold_in(own, 3), count)
    donor, receiver = mixed[0:count // 2 * 2:2], mixed[1:count // 2 * 2:2]
    margin = jnp.minimum(sizes[donor] - 1, most - sizes[receiver]) // 2
    margin = jnp.where((donor == order[0]) | (receiver == order[0]) | (sizes[receiver] == 0), 0, jnp.maximum(margin, 0))
    moved = jax.random.randint(jax.random.fold_in(own, 4), (count // 2,), 0, 1 << 20) % (margin + 1)
    sizes = sizes.at[donor].add(-moved).at[receiver].add(moved)
    members = jnp.searchsorted(jnp.cumsum(sizes), jnp.arange(rows * top), side="right").astype(jnp.int32)
    grid = members.reshape(top, rows).T
    grid = grid[jax.random.permutation(jax.random.fold_in(own, 1), rows)]
    offset_by = jax.random.randint(jax.random.fold_in(own, 2), (rows, 1), 0, top)
    return jnp.take_along_axis(grid, (jnp.arange(top)[None, :] + offset_by) % top, axis=1)


def shares(number_of, total, reach, slope, full):
    loads = [(1 << 20) // math.isqrt(rank ** slope) + 1 for rank in range(1, number_of + 1)]
    largest = reach if full else min(reach, max(-(-total // number_of), total * loads[0] // sum(loads)))
    least = 1 if total - largest >= number_of - 1 else 0
    holding, spare = [largest] + [least] * (number_of - 1), total - largest - least * (number_of - 1)
    while spare > 0:
        free = [i for i in range(1, number_of) if holding[i] < largest] or [i for i in range(1, number_of) if holding[i] < reach]
        pool, budget = sum([loads[i] for i in free]), spare
        for i in free:
            more = min(reach - holding[i], max(1, budget * loads[i] // pool), spare)
            holding[i] = holding[i] + more
            spare = spare - more
    return np.array(holding)


def setup_inputs(seed: int = 0, part: int = 0) -> dict:
    key_list = jax.random.split(jax.random.key(seed), 5)
    own_keys = jax.random.split(jax.random.fold_in(key_list[4], part), 5)
    queries = draw_queries(jax.random.fold_in(jax.random.fold_in(key_list[4], part), 71), part)
    passages = draw_passages(jax.random.fold_in(jax.random.fold_in(key_list[4], part), 71), part)
    first_blocks_keys = jax.random.split(jax.random.fold_in(own_keys[2], 1), QUERIES // Q_DEV)
    first_blocks_turns = jax.random.permutation(jax.random.fold_in(own_keys[2], 3), QUERIES // Q_DEV)
    first_blocks = jax.vmap(lambda own, number: shared_out(jax.random.fold_in(own_keys[2], 2), own, number, Q_DEV, NBLK, KB, CAP, 2))(first_blocks_keys, first_blocks_turns).reshape((QUERIES, KB))
    followup_blocks_keys = jax.random.split(jax.random.fold_in(own_keys[3], 1), QUERIES // Q_DEV)
    followup_blocks_turns = jax.random.permutation(jax.random.fold_in(own_keys[3], 3), QUERIES // Q_DEV)
    followup_blocks = jax.vmap(lambda own, number: shared_out(jax.random.fold_in(own_keys[3], 2), own, number, Q_DEV, NBLK, KB, CAP, 2))(followup_blocks_keys, followup_blocks_turns).reshape((QUERIES, KB))
    return {"queries": queries, "passages": passages, "first_blocks": first_blocks, "followup_blocks": followup_blocks}


SOFTMAX_HEAT = 2.0
FEEDBACK = 0.5


def one_group(packed, passages):
    cluster_query_rows, group_first, group_second = packed
    initial_round_rows = passages[group_first]
    match_scores = SOFTMAX_HEAT * jnp.einsum("dt,dbzt->dbz", cluster_query_rows, initial_round_rows, precision=lax.Precision.HIGHEST)
    flat_scores = match_scores.reshape(match_scores.shape[0], -1)
    weights = jax.nn.softmax(flat_scores, axis=1).reshape(match_scores.shape)
    feedback = jnp.einsum("gkr,gkre->ge", weights, initial_round_rows, precision=lax.Precision.HIGHEST)
    expanded = cluster_query_rows + (FEEDBACK * cluster_query_rows.shape[1] ** -0.5) * feedback
    second_rows = passages[group_second]
    second = jnp.einsum("dt,dbzt->dbz", expanded, second_rows, precision=lax.Precision.HIGHEST)
    return expanded, second


def reference(queries, passages, first_blocks, followup_blocks):
    groups = queries.shape[0] // 64
    packed = (queries.reshape(groups, 64, -1), first_blocks.reshape(groups, 64, -1), followup_blocks.reshape(groups, 64, -1))
    expanded, second = lax.map(partial(one_group, passages=passages), packed)
    return expanded.reshape(queries.shape), second.reshape(queries.shape[0], first_blocks.shape[1], -1)
```

```python
import functools

import jax
import jax.numpy as jnp
from jax import lax
from jax.experimental import pallas as pl
from jax.experimental.pallas import tpu as pltpu
from jax.sharding import PartitionSpec as P

SOFTMAX_HEAT = 2.0
FEEDBACK = 0.5
MASKED = -1e30
VMEM_BYTES = 50 * 1024 * 1024


def position_targets(block_ids, capacity):
    flat_ids = block_ids.reshape(-1)
    matches = flat_ids[:, None] == flat_ids[None, :]
    positions = jnp.arange(flat_ids.shape[0], dtype=jnp.int32)
    earlier = positions[None, :] < positions[:, None]
    ranking = jnp.sum(jnp.logical_and(matches, earlier), axis=1, dtype=jnp.int32)
    return flat_ids * capacity + ranking


def pack_rows(values, targets, owners, resident_blocks, capacity):
    buffer = jnp.zeros((owners * resident_blocks * capacity, values.shape[1]), values.dtype)
    buffer = buffer.at[targets].set(values)
    return buffer.reshape(owners, resident_blocks, capacity, values.shape[1])


def reply(results):
    return (
        lax.all_to_all(results[0], "cluster", split_axis=0, concat_axis=0, tiled=True),
        lax.all_to_all(results[1], "cluster", split_axis=0, concat_axis=0, tiled=True),
        lax.all_to_all(results[2], "cluster", split_axis=0, concat_axis=0, tiled=True),
    )


def send_back(match_scores):
    return lax.all_to_all(match_scores, "cluster", split_axis=0, concat_axis=0, tiled=True)


def local(queries, passages, first_blocks, followup_blocks):
    owners = lax.axis_size("cluster")
    resident_blocks = passages.shape[0]
    embed_width = queries.shape[1]
    per_query = first_blocks.shape[1]
    pair_count = queries.shape[0] * per_query
    all_blocks = owners * resident_blocks
    capacity = max(2, (3 * pair_count + 2 * all_blocks - 1) // (2 * all_blocks))
    coefficient = FEEDBACK * embed_width ** (-0.5)
    highest = lax.Precision.HIGHEST

    def project_onto_centroid(arrived):
        return jnp.einsum("nbce,bre->nbcr", arrived, passages, precision=highest)

    first_targets = position_targets(first_blocks, capacity)
    second_targets = position_targets(followup_blocks, capacity)
    repeated = jnp.repeat(queries, per_query, axis=0)
    first_sent = pack_rows(repeated, first_targets, owners, resident_blocks, capacity)
    match_scores = SOFTMAX_HEAT * project_onto_centroid(
        lax.all_to_all(first_sent, "cluster", split_axis=0, concat_axis=0, tiled=True)
    )
    highs = jnp.max(match_scores, axis=3)
    weights = jnp.exp(match_scores - highs[..., None])
    totals = jnp.sum(weights, axis=3)
    vectors = jnp.einsum("nbcr,bre->nbce", weights, passages, precision=highest)
    highs, totals, vectors = reply((highs, totals, vectors))
    highs = highs.reshape(-1)[first_targets].reshape(-1, per_query)
    totals = totals.reshape(-1)[first_targets].reshape(-1, per_query)
    vectors = vectors.reshape(-1, embed_width)[first_targets].reshape(-1, per_query, embed_width)
    peak_high = jnp.max(highs, axis=1, keepdims=True)
    scaled = jnp.exp(highs - peak_high)
    denominator = jnp.sum(scaled * totals, axis=1)
    feedback = jnp.einsum("qk,qke->qe", scaled, vectors, precision=highest) / denominator[:, None]
    expanded = queries + coefficient * feedback
    expanded_sent = pack_rows(
        jnp.repeat(expanded, per_query, axis=0), second_targets, owners, resident_blocks, capacity
    )
    returned = (lambda arrived: send_back(project_onto_centroid(arrived)))(
        lax.all_to_all(expanded_sent, "cluster", split_axis=0, concat_axis=0, tiled=True)
    )
    second_scores = returned.reshape(-1, returned.shape[3])[second_targets].reshape(
        queries.shape[0], per_query, -1
    )
    return (expanded, second_scores)


def dot_nt(a, b):
    return lax.dot_general(a, b, (((1,), (1,)), ((), ())), preferred_element_type=jnp.float32)


def dot_nn(a, b):
    return lax.dot_general(a, b, (((1,), (0,)), ((), ())), preferred_element_type=jnp.float32)


def halves(x):
    high = x.astype(jnp.bfloat16)
    return high, (x - high.astype(jnp.float32)).astype(jnp.bfloat16)


def ring_kernel(
    chips, queries_in, passages, first_in, followup_in, expanded, scores,
    first, followup, corpus, turned_hi, turned_lo, queries, pair, total, asked, chosen, picked,
    load_sem, send_r, recv_r, send_l, recv_l, send_a, recv_a, send_b, recv_b,
):
    me = lax.axis_index("cluster")
    chip, core = me // 2, me % 2
    rows, width = queries.shape
    top = first.shape[0]
    size = passages.shape[1]
    piece = size // 2
    half = chips // 2
    last = chips - 1
    spot = (1 - chip % 2) * (chip // 2) + (chip % 2) * (chips - 1 - chip // 2)

    def chip_at(position):
        position = (position + chips) % chips
        late = position // half
        return (1 - late) * (2 * position) + late * (2 * (chips - 1 - position) + 1)

    right = 2 * chip_at(spot + 1) + core
    left = 2 * chip_at(spot + chips - 1) + core
    other = 2 * chip + 1 - core

    def remote(src, dst, send, recv, device):
        return pltpu.make_async_remote_copy(
            src_ref=src, dst_ref=dst, send_sem=send, recv_sem=recv,
            device_id={"cluster": device}, device_id_type=pl.DeviceIdType.MESH,
        )

    def rightward(step, src):
        return remote(src, corpus.at[step, 0], send_r.at[step], recv_r.at[step], right)

    def leftward(step, src):
        return remote(src, corpus.at[step, 1], send_l.at[step], recv_l.at[step], left)

    def across_a(step):
        return remote(corpus.at[step, 0], corpus.at[step, 2], send_a.at[step], recv_a.at[step], other)

    def across_b(step):
        return remote(corpus.at[step, 1], corpus.at[step, 3], send_b.at[step], recv_b.at[step], other)

    def ends(h):
        part = pl.ds(h * piece, piece)
        return (
            remote(
                corpus.at[last - 2, 0, part], corpus.at[last, 0, part],
                send_r.at[last + h], recv_r.at[last + h], right,
            ),
            remote(
                corpus.at[last - 2, 1, part], corpus.at[last, 1, part],
                send_l.at[last + h], recv_l.at[last + h], left,
            ),
        )

    def ends_across(h):
        part = pl.ds(h * piece, piece)
        return (
            remote(
                corpus.at[last, 0, part], corpus.at[last, 2, part],
                send_a.at[last + h], recv_a.at[last + h], other,
            ),
            remote(
                corpus.at[last, 1, part], corpus.at[last, 3, part],
                send_b.at[last + h], recv_b.at[last + h], other,
            ),
        )

    def blocks_of(step):
        away = (step + 1) // 2
        from_left = 2 * chip_at(spot + chips - away)
        from_right = 2 * chip_at(spot + away)
        a, b = (step + 1) % 2, step % 2
        return (
            (from_left + core) * 2 + a,
            (from_right + core) * 2 + b,
            (from_left + 1 - core) * 2 + a,
            (from_right + 1 - core) * 2 + b,
        )

    loads = (
        pltpu.make_async_copy(passages.at[1], corpus.at[0, 0], load_sem.at[0]),
        pltpu.make_async_copy(passages.at[0], corpus.at[0, 1], load_sem.at[1]),
        pltpu.make_async_copy(queries_in, queries, load_sem.at[2]),
        pltpu.make_async_copy(first_in, first, load_sem.at[3]),
        pltpu.make_async_copy(followup_in, followup, load_sem.at[4]),
    )
    for load in loads:
        load.start()
    barrier = pltpu.get_barrier_semaphore()
    for device in (right, left, other):
        pl.semaphore_signal(
            barrier, inc=1, device_id={"cluster": device}, device_id_type=pl.DeviceIdType.MESH
        )
    pl.semaphore_wait(barrier, 3)
    for load in loads[:2]:
        load.wait()
    rightward(1, corpus.at[0, 1]).start()
    leftward(1, corpus.at[0, 0]).start()
    for load in loads[2:]:
        load.wait()

    def put_pair(x):
        high, low = halves(x)
        pair[pl.ds(0, rows), :] = high
        pair[pl.ds(rows, rows), :] = low

    put_pair(queries[...])
    total[...] = jnp.zeros_like(total)
    for j in range(top):
        asked[j] = jnp.broadcast_to(first[j : j + 1, :].astype(jnp.float32), (size, rows)).T
        chosen[j] = jnp.broadcast_to(followup[j : j + 1, :].astype(jnp.float32), (size, rows)).T
    picked[...] = jnp.zeros_like(picked)
    lane = lax.broadcasted_iota(jnp.int32, (1, size), 1)

    def absorb(sources, place, names, carry):
        peak, norm = carry
        split = [halves(source[...]) for source in sources]
        high = jnp.concatenate([h for h, _ in split], axis=0)
        low = jnp.concatenate([l for _, l in split], axis=0)
        place[0][...] = high.T
        place[1][...] = low.T
        both = dot_nn(pair[...], place[0][...])
        found = SOFTMAX_HEAT * (
            both[:rows] + both[rows:] + dot_nn(pair[pl.ds(0, rows), :], place[1][...])
        )
        parts, hits = [], []
        top_score = peak
        for t, name in enumerate(names):
            hit = asked[0] == name
            for j in range(1, top):
                hit = jnp.logical_or(hit, asked[j] == name)
            part = jnp.where(hit, found[:, t * size : (t + 1) * size], MASKED)
            top_score = jnp.maximum(top_score, jnp.max(part, axis=1, keepdims=True))
            parts.append(part)
            hits.append(hit)
        shrink = jnp.exp(peak - top_score)
        weights = jnp.concatenate(
            [jnp.where(hit, jnp.exp(part - top_score), 0.0) for hit, part in zip(hits, parts)], axis=1
        )
        norm = norm * shrink + jnp.sum(weights, axis=1, keepdims=True)
        first_half, second_half = halves(weights)
        mixed = dot_nn(jnp.concatenate([first_half, second_half], axis=0), high)
        total[...] = total[...] * shrink + (mixed[:rows] + mixed[rows:] + dot_nn(first_half, low))
        return top_score, norm

    def whole(step, slot, carry):
        sources = [corpus.at[step, t] for t in (slot, slot + 1)]
        place = (turned_hi.at[step, slot // 2], turned_lo.at[step, slot // 2])
        names = [block.astype(jnp.float32) for block in blocks_of(step)[slot : slot + 2]]
        return absorb(sources, place, names, carry)

    def partial(h, slot, carry):
        sources = [corpus.at[last, t, pl.ds(h * piece, piece)] for t in (slot, slot + 1)]
        spread = pl.ds(h * size, size)
        place = (
            turned_hi.at[last, slot // 2, :, spread],
            turned_lo.at[last, slot // 2, :, spread],
        )
        a, b = (block.astype(jnp.float32) for block in blocks_of(last)[slot : slot + 2])
        return absorb(sources, place, [jnp.where(lane < piece, a, b)], carry)

    def first_round(step, carry):
        @pl.when(step > 0)
        def _():
            rightward(step, corpus.at[step, 0]).wait_recv()
            leftward(step, corpus.at[step, 1]).wait_recv()

        @pl.when(step < last - 2)
        def _():
            rightward(step + 2, corpus.at[step, 0]).start()
            leftward(step + 2, corpus.at[step, 1]).start()

        @pl.when(step == last - 2)
        def _():
            for h in range(2):
                for copy in ends(h):
                    copy.start()

        across_a(step).start()
        across_b(step).start()
        carry = whole(step, 0, carry)
        across_a(step).wait_recv()
        across_b(step).wait_recv()
        return whole(step, 2, carry)

    carry = (jnp.full((rows, 1), MASKED, jnp.float32), jnp.zeros((rows, 1), jnp.float32))
    carry = lax.fori_loop(0, last, first_round, carry)
    for h in range(2):
        for copy in ends(h):
            copy.wait_recv()
        for copy in ends_across(h):
            copy.start()
        carry = partial(h, 0, carry)
        for copy in ends_across(h):
            copy.wait_recv()
        carry = partial(h, 2, carry)
    norm = carry[1]

    after = queries[...] + (FEEDBACK * width ** (-0.5)) * (total[...] / norm)
    expanded[...] = after
    put_pair(after)

    def score(step, s):
        both = dot_nn(pair[...], turned_hi[step, s])
        return both[:rows] + both[rows:] + dot_nn(pair[pl.ds(0, rows), :], turned_lo[step, s])

    def pick(values, names):
        for j in range(top):
            value = picked[j]
            for name, found in zip(names, values):
                value = jnp.where(chosen[j] == name, found, value)
            picked[j] = value

    def second_round(step, carry):
        ids = [block.astype(jnp.float32) for block in blocks_of(step)]
        for s in range(2):
            found = score(step, s)
            pick([found[:, :size], found[:, size:]], ids[2 * s : 2 * s + 2])
        return carry

    lax.fori_loop(0, last, second_round, 0)
    ids = [block.astype(jnp.float32) for block in blocks_of(last)]
    for s in range(2):
        found = score(last, s)
        a, b = found[:, :size], found[:, size:]
        early = jnp.where(lane < piece, a, pltpu.roll(b, piece, 1))
        late = jnp.where(lane < piece, pltpu.roll(a, piece, 1), b)
        pick([early, late], ids[2 * s : 2 * s + 2])
    for j in range(top):
        scores[:, j, :] = picked[j]

    def drain(step, carry):
        @pl.when(step > 0)
        def _():
            rightward(step, corpus.at[step, 0]).wait_send()
            leftward(step, corpus.at[step, 1]).wait_send()

        across_a(step).wait_send()
        across_b(step).wait_send()
        return carry

    lax.fori_loop(0, last, drain, 0)
    for h in range(2):
        for copy in ends(h) + ends_across(h):
            copy.wait_send()


def grant_of(queries, passages, first_blocks):
    resident, size, width = passages.shape
    rows = queries.shape[0]
    corpus = lax.axis_size("cluster") * resident * size * width * 8
    return corpus + (10 * rows * width + 6 * first_blocks.shape[1] * rows * size) * 4


def ring_fits(queries, passages, first_blocks):
    owners = lax.axis_size("cluster")
    resident, size, _ = passages.shape
    fits = grant_of(queries, passages, first_blocks) < VMEM_BYTES
    return owners % 4 == 0 and resident == 2 and fits and queries.shape[0] == size


def device_program(queries, passages, first_blocks, followup_blocks):
    if not ring_fits(queries, passages, first_blocks):
        return local(queries, passages, first_blocks, followup_blocks)
    chips = lax.axis_size("cluster") // 2
    rows, width = queries.shape
    size = passages.shape[1]
    top = first_blocks.shape[1]
    vmem = pl.BlockSpec(memory_space=pltpu.VMEM)
    hbm = pl.BlockSpec(memory_space=pltpu.HBM)
    return pl.pallas_call(
        functools.partial(ring_kernel, chips),
        out_shape=(
            jax.ShapeDtypeStruct((rows, width), jnp.float32),
            jax.ShapeDtypeStruct((rows, top, size), jnp.float32),
        ),
        in_specs=[hbm, hbm, hbm, hbm],
        out_specs=(vmem, vmem),
        scratch_shapes=[
            pltpu.VMEM((top, rows), jnp.int32),
            pltpu.VMEM((top, rows), jnp.int32),
            pltpu.VMEM((chips, 4, size, width), jnp.float32),
            pltpu.VMEM((chips, 2, width, 2 * size), jnp.bfloat16),
            pltpu.VMEM((chips, 2, width, 2 * size), jnp.bfloat16),
            pltpu.VMEM((rows, width), jnp.float32),
            pltpu.VMEM((2 * rows, width), jnp.bfloat16),
            pltpu.VMEM((rows, width), jnp.float32),
            pltpu.VMEM((top, rows, size), jnp.float32),
            pltpu.VMEM((top, rows, size), jnp.float32),
            pltpu.VMEM((top, rows, size), jnp.float32),
            pltpu.SemaphoreType.DMA((5,)),
        ]
        + [pltpu.SemaphoreType.DMA((chips + 1,))] * 8,
        compiler_params=pltpu.CompilerParams(
            collective_id=0, has_side_effects=True, vmem_limit_bytes=VMEM_BYTES
        ),
    )(*[pltpu.with_memory_space_constraint(x, pltpu.HBM) for x in (queries, passages, first_blocks.T, followup_blocks.T)])


def solution(mesh):
    return jax.shard_map(
        device_program,
        mesh=mesh,
        in_specs=(
            P(("parts", "cluster"), None),
            P(("parts", "cluster"), None, None),
            P(("parts", "cluster"), None),
            P(("parts", "cluster"), None),
        ),
        out_specs=(P(("parts", "cluster"), None), P(("parts", "cluster"), None, None)),
        check_vma=False,
    )
```

```python
import functools

import jax
import jax.numpy as jnp
from jax import lax
from jax.experimental import pallas as pl
from jax.experimental.pallas import tpu as pltpu
from jax.sharding import PartitionSpec as P

SOFTMAX_HEAT = 2.0
FEEDBACK = 0.5
MASKED = -1e30
VMEM_BYTES = 50 * 1024 * 1024


def position_targets(block_ids, capacity):
    flat_ids = block_ids.reshape(-1)
    matches = flat_ids[:, None] == flat_ids[None, :]
    positions = jnp.arange(flat_ids.shape[0], dtype=jnp.int32)
    earlier = positions[None, :] < positions[:, None]
    ranking = jnp.sum(jnp.logical_and(matches, earlier), axis=1, dtype=jnp.int32)
    return flat_ids * capacity + ranking


def pack_rows(values, targets, owners, resident_blocks, capacity):
    buffer = jnp.zeros((owners * resident_blocks * capacity, values.shape[1]), values.dtype)
    buffer = buffer.at[targets].set(values)
    return buffer.reshape(owners, resident_blocks, capacity, values.shape[1])


def reply(results):
    return (
        lax.all_to_all(results[0], "cluster", split_axis=0, concat_axis=0, tiled=True),
        lax.all_to_all(results[1], "cluster", split_axis=0, concat_axis=0, tiled=True),
        lax.all_to_all(results[2], "cluster", split_axis=0, concat_axis=0, tiled=True),
    )


def send_back(match_scores):
    return lax.all_to_all(match_scores, "cluster", split_axis=0, concat_axis=0, tiled=True)


def local(queries, passages, first_blocks, followup_blocks):
    owners = lax.axis_size("cluster")
    resident_blocks = passages.shape[0]
    embed_width = queries.shape[1]
    per_query = first_blocks.shape[1]
    pair_count = queries.shape[0] * per_query
    all_blocks = owners * resident_blocks
    capacity = max(2, (3 * pair_count + 2 * all_blocks - 1) // (2 * all_blocks))
    coefficient = FEEDBACK * embed_width ** (-0.5)
    highest = lax.Precision.HIGHEST

    def project_onto_centroid(arrived):
        return jnp.einsum("nbce,bre->nbcr", arrived, passages, precision=highest)

    first_targets = position_targets(first_blocks, capacity)
    second_targets = position_targets(followup_blocks, capacity)
    repeated = jnp.repeat(queries, per_query, axis=0)
    first_sent = pack_rows(repeated, first_targets, owners, resident_blocks, capacity)
    match_scores = SOFTMAX_HEAT * project_onto_centroid(
        lax.all_to_all(first_sent, "cluster", split_axis=0, concat_axis=0, tiled=True)
    )
    highs = jnp.max(match_scores, axis=3)
    weights = jnp.exp(match_scores - highs[..., None])
    totals = jnp.sum(weights, axis=3)
    vectors = jnp.einsum("nbcr,bre->nbce", weights, passages, precision=highest)
    highs, totals, vectors = reply((highs, totals, vectors))
    highs = highs.reshape(-1)[first_targets].reshape(-1, per_query)
    totals = totals.reshape(-1)[first_targets].reshape(-1, per_query)
    vectors = vectors.reshape(-1, embed_width)[first_targets].reshape(-1, per_query, embed_width)
    peak_high = jnp.max(highs, axis=1, keepdims=True)
    scaled = jnp.exp(highs - peak_high)
    denominator = jnp.sum(scaled * totals, axis=1)
    feedback = jnp.einsum("qk,qke->qe", scaled, vectors, precision=highest) / denominator[:, None]
    expanded = queries + coefficient * feedback
    expanded_sent = pack_rows(
        jnp.repeat(expanded, per_query, axis=0), second_targets, owners, resident_blocks, capacity
    )
    returned = (lambda arrived: send_back(project_onto_centroid(arrived)))(
        lax.all_to_all(expanded_sent, "cluster", split_axis=0, concat_axis=0, tiled=True)
    )
    second_scores = returned.reshape(-1, returned.shape[3])[second_targets].reshape(
        queries.shape[0], per_query, -1
    )
    return (expanded, second_scores)


def dot_nt(a, b):
    return lax.dot_general(a, b, (((1,), (1,)), ((), ())), preferred_element_type=jnp.float32)


def dot_nn(a, b):
    return lax.dot_general(a, b, (((1,), (0,)), ((), ())), preferred_element_type=jnp.float32)


def halves(x):
    high = x.astype(jnp.bfloat16)
    return high, (x - high.astype(jnp.float32)).astype(jnp.bfloat16)


def hub_kernel(
    queries_in, passages, first_in, followup_in, expanded, scores,
    first, followup, corpus, turned_hi, turned_lo, queries, pair, total, asked, chosen, picked,
    expanded_out, scores_out,
    load_sem, send_c, recv_c, send_y, recv_y, send_z, recv_z, send_x, recv_x, send_back, recv_back,
):
    me = lax.axis_index("cluster")
    core, y, z = me % 2, (me // 2) % 2, me // 4
    rows, width = expanded.shape
    both_rows = 2 * rows
    top, _, size = asked.shape
    piece = size // 2
    inner = ((z + 1) % 4) // 2
    mate_z = z + 1 - 2 * (z % 2)
    far_z = 3 - z
    far_mate_z = far_z + 1 - 2 * (far_z % 2)

    def device(zz, yy, cc):
        return (2 * zz + yy) * 2 + cc

    mate = device(mate_z, y, core)
    beside = device(z, 1 - y, core)
    far = device(far_z, y, core)
    other = device(z, y, 1 - core)

    plan = (
        (z, y, 0), (z, y, 1),
        (mate_z, y, 0), (mate_z, y, 1), (mate_z, 1 - y, 1), (mate_z, 1 - y, 0),
        (z, 1 - y, 0), (z, 1 - y, 1), (far_z, 1 - y, 0), (far_z, 1 - y, 1), (far_mate_z, 1 - y, 0),
        (far_z, y, 0), (far_z, y, 1), (far_mate_z, y, 0), (far_mate_z, y, 1), (far_mate_z, 1 - y, 1),
    )

    def names_of(unit):
        chip, index = 0, 0
        for k, (zz, yy, ii) in enumerate(plan):
            here = jnp.int32(unit == k) if isinstance(unit, int) else (unit == k).astype(jnp.int32)
            chip = chip + here * (2 * zz + yy)
            index = index + here * ii
        return (
            ((2 * chip + core) * 2 + index).astype(jnp.float32),
            ((2 * chip + 1 - core) * 2 + index).astype(jnp.float32),
        )

    def remote(src, dst, send, recv, target):
        return pltpu.make_async_remote_copy(
            src_ref=src, dst_ref=dst, send_sem=send, recv_sem=recv,
            device_id={"cluster": target}, device_id_type=pl.DeviceIdType.MESH,
        )

    def part(h):
        return pl.ds(h * piece, piece)

    def unit_copy(source, unit, sems, k, target):
        return remote(corpus.at[source, 0], corpus.at[unit, 0], sems[0].at[k], sems[1].at[k], target)

    def half_copy(source, unit, h, sems, k, target):
        return remote(
            corpus.at[source, 0, part(h)], corpus.at[unit, 0, part(h)],
            sems[0].at[k], sems[1].at[k], target,
        )

    on_c, on_y, on_z, on_x = (send_c, recv_c), (send_y, recv_y), (send_z, recv_z), (send_x, recv_x)

    def ids_up(k):
        held = (first, followup)[k]
        return remote(held.at[0], held.at[1], send_c.at[k], recv_c.at[k], mate)

    def queries_up():
        return remote(
            queries.at[pl.ds(0, rows)], queries.at[pl.ds(rows, rows)], send_c.at[2], recv_c.at[2], mate
        )

    def up(unit, h):
        source = unit - 2 if isinstance(unit, int) and unit < 4 else unit
        return half_copy(source, unit, h, on_c, 2 * unit + h, mate)

    def side(unit):
        return unit_copy(unit - 3 if isinstance(unit, int) and unit > 7 else unit, unit, on_y, unit, beside)

    def across(unit):
        return remote(corpus.at[unit, 0], corpus.at[unit, 1], send_x.at[unit], recv_x.at[unit], other)

    def across_half(unit, h):
        k = 16 + (unit // 5 - 1) * 2 + h
        return remote(
            corpus.at[unit, 0, part(h)], corpus.at[unit, 1, part(h)], send_x.at[k], recv_x.at[k], other
        )

    def back(k):
        source, target = ((expanded_out, expanded), (scores_out, scores))[k]
        return remote(source, target, send_back.at[k], recv_back.at[k], mate)

    loads = (
        pltpu.make_async_copy(passages.at[0], corpus.at[0, 0], load_sem.at[0]),
        pltpu.make_async_copy(passages.at[1], corpus.at[1, 0], load_sem.at[1]),
        pltpu.make_async_copy(queries_in, queries.at[pl.ds(0, rows)], load_sem.at[2]),
        pltpu.make_async_copy(first_in, first.at[0], load_sem.at[3]),
        pltpu.make_async_copy(followup_in, followup.at[0], load_sem.at[4]),
    )
    for load in loads:
        load.start()
    barrier = pltpu.get_barrier_semaphore()
    for target in (mate, beside, other):
        pl.semaphore_signal(
            barrier, inc=1, device_id={"cluster": target}, device_id_type=pl.DeviceIdType.MESH
        )

    @pl.when(inner == 1)
    def _():
        pl.semaphore_signal(
            barrier, inc=1, device_id={"cluster": far}, device_id_type=pl.DeviceIdType.MESH
        )

    pl.semaphore_wait(barrier, 3 + inner)
    for load in loads:
        load.wait()

    @pl.when(inner == 0)
    def _():
        ids_up(0).start()
        ids_up(1).start()
        queries_up().start()
        corner_side = [
            remote(corpus.at[k, 0], corpus.at[5 - k, 0], send_y.at[k], recv_y.at[k], beside)
            for k in (1, 0)
        ]
        for copy in corner_side:
            copy.start()
        for unit in (2, 3):
            for h in range(2):
                up(unit, h).start()
        for copy, unit in zip(corner_side, (4, 5)):
            copy.wait_recv()
            for h in range(2):
                up(unit, h).start()
        for k in range(2):
            back(k).wait_recv()
        ids_up(0).wait_send()
        ids_up(1).wait_send()
        queries_up().wait_send()
        for copy in corner_side:
            copy.wait_send()
        for unit in (2, 3, 4, 5):
            for h in range(2):
                up(unit, h).wait_send()

    @pl.when(inner == 1)
    def _():
        hub(
            first, followup, corpus, turned_hi, turned_lo, queries, pair, total, asked, chosen,
            picked, expanded, scores, expanded_out, scores_out,
            names_of, unit_copy, half_copy, ids_up, queries_up, across, across_half, back, part,
            on_c, on_y, on_z, mate, beside, far,
        )


def hub(
    first, followup, corpus, turned_hi, turned_lo, queries, pair, total, asked, chosen,
    picked, expanded, scores, expanded_out, scores_out,
    names_of, unit_copy, half_copy, ids_up, queries_up, across, across_half, back, part,
    on_c, on_y, on_z, mate, beside, far,
):
    rows, width = expanded.shape
    both_rows = 2 * rows
    top, _, size = asked.shape
    piece = size // 2
    lane = lax.broadcasted_iota(jnp.int32, (1, size), 1)

    def from_mate(unit, h):
        return half_copy(unit, unit, h, on_c, 2 * unit + h, mate)

    def from_side(t):
        return unit_copy(5 + t, 5 + t, on_y, 5 + t, beside)

    def last_side(h):
        return half_copy(13, 10, h, on_y, 10 + h, beside)

    def own_side(k):
        return unit_copy(k, 6 + k, on_y, 6 + k, beside)

    def pass_side(t):
        return unit_copy(10 + t, 7 + t, on_y, 7 + t, beside)

    def own_far(k):
        return unit_copy(k, 11 + k, on_z, k, far)

    def pass_far(t, h):
        return half_copy(t, 11 + t, h, on_z, 2 * t + h, far)

    def from_far(t):
        return unit_copy(10 + t, 10 + t, on_z, t - 1, far)

    def from_far_half(t, h):
        return half_copy(10 + t, 10 + t, h, on_z, 2 * (t - 1) + h, far)

    for k in range(2):
        own_far(k).start()
        own_side(k).start()
    for k in range(2):
        across(k).start()
    from_far(1).wait_recv()
    pass_side(1).start()
    across(11).start()
    from_side(1).wait_recv()
    across(6).start()
    for k in range(2):
        ids_up(k).wait_recv()
    queries_up().wait_recv()

    def put_pair(x):
        high, low = halves(x)
        pair[pl.ds(0, both_rows), :] = high
        pair[pl.ds(both_rows, both_rows), :] = low

    def dot_three(high, low, right_high, right_low):
        return dot_nn(high, right_high) + (dot_nn(low, right_high) + dot_nn(high, right_low))

    put_pair(queries[...])
    total[...] = jnp.zeros_like(total)
    picked[...] = jnp.zeros_like(picked)
    for g in range(2):
        group = pl.ds(g * rows, rows)
        for j in range(top):
            for held, spread in ((first, asked), (followup, chosen)):
                line = held[g, j : j + 1, :].astype(jnp.float32)
                spread[j, group, :] = jnp.broadcast_to(line, (size, rows)).T

    def absorb(pieces, carry):
        peak, norm = carry
        highs, lows, names = [], [], []
        for unit, h in pieces:
            high, low = halves(
                jnp.concatenate([corpus[unit, 0, part(h), :], corpus[unit, 1, part(h), :]], axis=0)
            )
            place = pl.ds(h * size, size)
            turned_hi[unit, :, place] = high.T
            turned_lo[unit, :, place] = low.T
            highs.append(high)
            lows.append(low)
            own, others = names_of(unit)
            names.append(jnp.where(lane < piece, own, others))
        wide = [
            jnp.concatenate([turned[unit, :, pl.ds(h * size, size)] for unit, h in pieces], axis=1)
            for turned in (turned_hi, turned_lo)
        ]
        all_found = dot_three(
            pair[pl.ds(0, both_rows), :], pair[pl.ds(both_rows, both_rows), :], *wide
        )
        sums = [all_found[:, k * size : (k + 1) * size] for k in range(len(pieces))]
        parts, hits = [], []
        top_score = peak
        for name, found in zip(names, sums):
            hit = asked[0] == name
            for j in range(1, top):
                hit = jnp.logical_or(hit, asked[j] == name)
            score = jnp.where(hit, SOFTMAX_HEAT * found, MASKED)
            top_score = jnp.maximum(top_score, jnp.max(score, axis=1, keepdims=True))
            parts.append(score)
            hits.append(hit)
        shrink = jnp.exp(peak - top_score)
        weights = jnp.concatenate(
            [jnp.where(hit, jnp.exp(score - top_score), 0.0) for hit, score in zip(hits, parts)], axis=1
        )
        norm = norm * shrink + jnp.sum(weights, axis=1, keepdims=True)
        weight_high, weight_low = halves(weights)
        mixed = dot_three(
            weight_high, weight_low, jnp.concatenate(highs, axis=0), jnp.concatenate(lows, axis=0)
        )
        total[...] = total[...] * shrink + mixed
        return top_score, norm

    def take(unit, carry):
        across(unit).wait_recv()
        return absorb([(unit, 0), (unit, 1)], carry)

    def step(t, carry):
        carry = take(4 + t, carry)
        carry = take(t - 1, carry)
        from_mate(t, 0).wait_recv()

        @pl.when(t < 5)
        def _():
            pass_far(t, 0).start()

        carry = take(9 + t, carry)

        @pl.when(t < 5)
        def _():
            from_mate(t, 1).wait_recv()
            pass_far(t, 1).start()
            across(t).start()
            from_side(t).wait_recv()
            across(5 + t).start()

            @pl.when(t == 2)
            def _():
                from_far(t).wait_recv()
                pass_side(t).start()

            @pl.when(t > 2)
            def _():
                for h in range(2):
                    from_far_half(t, h).wait_recv()

            across(10 + t).start()

            @pl.when(t == 3)
            def _():
                for h in range(2):
                    last_side(h).start()

        return carry

    carry = (
        jnp.full((both_rows, 1), MASKED, jnp.float32), jnp.zeros((both_rows, 1), jnp.float32)
    )
    carry = take(0, carry)
    carry = lax.fori_loop(2, 6, step, carry)

    def finish(h, carry):
        @pl.when(h == 1)
        def _():
            from_mate(5, h).wait_recv()

        across_half(5, h).start()
        last_side(h).wait_recv()
        across_half(10, h).start()
        from_far_half(5, h).wait_recv()
        across_half(15, h).start()
        for unit in (5, 10, 15):
            across_half(unit, h).wait_recv()
        return absorb([(5, h), (10, h), (15, h)], carry)

    _, norm = lax.fori_loop(0, 2, finish, carry)

    after = queries[...] + (FEEDBACK * width ** (-0.5)) * (total[...] / norm)
    expanded_out[...] = after[rows:]
    expanded[...] = after[:rows]
    put_pair(after)
    back(0).start()

    def second_round(unit, carry):
        found = dot_three(
            pair[pl.ds(0, both_rows), :], pair[pl.ds(both_rows, both_rows), :],
            turned_hi[unit], turned_lo[unit],
        )
        a, b = found[:, :size], found[:, size:]
        own = jnp.where(lane < piece, a, pltpu.roll(b, piece, 1))
        others = jnp.where(lane < piece, pltpu.roll(a, piece, 1), b)
        names = names_of(unit)
        for j in range(top):
            value = jnp.where(chosen[j] == names[0], own, picked[j])
            picked[j] = jnp.where(chosen[j] == names[1], others, value)
        return carry

    lax.fori_loop(0, 16, second_round, 0)
    for j in range(top):
        scores_out[:, j, :] = picked[j, pl.ds(rows, rows), :]
    for j in range(top):
        scores[:, j, :] = picked[j, pl.ds(0, rows), :]
    back(1).start()

    for k in range(2):
        own_far(k).wait_send()
        own_side(k).wait_send()
        pass_side(1 + k).wait_send()
        last_side(k).wait_send()
        back(k).wait_send()

    def drain(t, carry):
        for h in range(2):
            pass_far(t, h).wait_send()
        return carry

    lax.fori_loop(2, 5, drain, 0)

    def drain_across(unit, carry):
        @pl.when(unit % 5 != 0)
        def _():
            across(unit).wait_send()

        return carry

    across(0).wait_send()
    lax.fori_loop(1, 15, drain_across, 0)
    for unit in (5, 10, 15):
        for h in range(2):
            across_half(unit, h).wait_send()


def grant_of(queries, passages, first_blocks):
    resident, size, width = passages.shape
    rows = queries.shape[0]
    corpus = lax.axis_size("cluster") * resident * size * width * 8
    return corpus + (12 * rows * width + 10 * first_blocks.shape[1] * rows * size) * 4


def hub_fits(queries, passages, first_blocks):
    owners = lax.axis_size("cluster")
    resident, size, _ = passages.shape
    fits = grant_of(queries, passages, first_blocks) < VMEM_BYTES
    return owners == 16 and resident == 2 and fits and queries.shape[0] == size


def device_program(queries, passages, first_blocks, followup_blocks):
    if not hub_fits(queries, passages, first_blocks):
        return local(queries, passages, first_blocks, followup_blocks)
    units = lax.axis_size("cluster")
    rows, width = queries.shape
    size = passages.shape[1]
    top = first_blocks.shape[1]
    vmem = pl.BlockSpec(memory_space=pltpu.VMEM)
    hbm = pl.BlockSpec(memory_space=pltpu.HBM)
    operands = (queries, passages, first_blocks.T, followup_blocks.T)
    dma = pltpu.SemaphoreType.DMA
    return pl.pallas_call(
        hub_kernel,
        out_shape=(
            jax.ShapeDtypeStruct((rows, width), jnp.float32),
            jax.ShapeDtypeStruct((rows, top, size), jnp.float32),
        ),
        in_specs=[hbm, hbm, hbm, hbm],
        out_specs=(vmem, vmem),
        scratch_shapes=[
            pltpu.VMEM((2, top, rows), jnp.int32),
            pltpu.VMEM((2, top, rows), jnp.int32),
            pltpu.VMEM((units, 2, size, width), jnp.float32),
            pltpu.VMEM((units, width, 2 * size), jnp.bfloat16),
            pltpu.VMEM((units, width, 2 * size), jnp.bfloat16),
            pltpu.VMEM((2 * rows, width), jnp.float32),
            pltpu.VMEM((4 * rows, width), jnp.bfloat16),
            pltpu.VMEM((2 * rows, width), jnp.float32),
            pltpu.VMEM((top, 2 * rows, size), jnp.float32),
            pltpu.VMEM((top, 2 * rows, size), jnp.float32),
            pltpu.VMEM((top, 2 * rows, size), jnp.float32),
            pltpu.VMEM((rows, width), jnp.float32),
            pltpu.VMEM((rows, top, size), jnp.float32),
            dma((5,)),
            dma((12,)), dma((12,)),
            dma((12,)), dma((12,)),
            dma((10,)), dma((10,)),
            dma((22,)), dma((22,)),
            dma((2,)), dma((2,)),
        ],
        compiler_params=pltpu.CompilerParams(
            collective_id=0, has_side_effects=True, vmem_limit_bytes=VMEM_BYTES
        ),
    )(*[pltpu.with_memory_space_constraint(x, pltpu.HBM) for x in operands])


def solution(mesh):
    return jax.shard_map(
        device_program,
        mesh=mesh,
        in_specs=(
            P(("parts", "cluster"), None),
            P(("parts", "cluster"), None, None),
            P(("parts", "cluster"), None),
            P(("parts", "cluster"), None),
        ),
        out_specs=(P(("parts", "cluster"), None), P(("parts", "cluster"), None, None)),
        check_vma=False,
    )
```

```python
import functools

import jax
import jax.numpy as jnp
from jax import lax
from jax.experimental import pallas as pl
from jax.experimental.pallas import tpu as pltpu
from jax.sharding import PartitionSpec as P

SOFTMAX_HEAT = 2.0
FEEDBACK = 0.5
MASKED = -1e30
VMEM_BYTES = 50 * 1024 * 1024


def position_targets(block_ids, capacity):
    flat_ids = block_ids.reshape(-1)
    matches = flat_ids[:, None] == flat_ids[None, :]
    positions = jnp.arange(flat_ids.shape[0], dtype=jnp.int32)
    earlier = positions[None, :] < positions[:, None]
    ranking = jnp.sum(jnp.logical_and(matches, earlier), axis=1, dtype=jnp.int32)
    return flat_ids * capacity + ranking


def pack_rows(values, targets, owners, resident_blocks, capacity):
    buffer = jnp.zeros((owners * resident_blocks * capacity, values.shape[1]), values.dtype)
    buffer = buffer.at[targets].set(values)
    return buffer.reshape(owners, resident_blocks, capacity, values.shape[1])


def reply(results):
    return (
        lax.all_to_all(results[0], "cluster", split_axis=0, concat_axis=0, tiled=True),
        lax.all_to_all(results[1], "cluster", split_axis=0, concat_axis=0, tiled=True),
        lax.all_to_all(results[2], "cluster", split_axis=0, concat_axis=0, tiled=True),
    )


def send_back(match_scores):
    return lax.all_to_all(match_scores, "cluster", split_axis=0, concat_axis=0, tiled=True)


def local(queries, passages, first_blocks, followup_blocks):
    owners = lax.axis_size("cluster")
    resident_blocks = passages.shape[0]
    embed_width = queries.shape[1]
    per_query = first_blocks.shape[1]
    pair_count = queries.shape[0] * per_query
    all_blocks = owners * resident_blocks
    capacity = max(2, (3 * pair_count + 2 * all_blocks - 1) // (2 * all_blocks))
    coefficient = FEEDBACK * embed_width ** (-0.5)
    highest = lax.Precision.HIGHEST

    def project_onto_centroid(arrived):
        return jnp.einsum("nbce,bre->nbcr", arrived, passages, precision=highest)

    first_targets = position_targets(first_blocks, capacity)
    second_targets = position_targets(followup_blocks, capacity)
    repeated = jnp.repeat(queries, per_query, axis=0)
    first_sent = pack_rows(repeated, first_targets, owners, resident_blocks, capacity)
    match_scores = SOFTMAX_HEAT * project_onto_centroid(
        lax.all_to_all(first_sent, "cluster", split_axis=0, concat_axis=0, tiled=True)
    )
    highs = jnp.max(match_scores, axis=3)
    weights = jnp.exp(match_scores - highs[..., None])
    totals = jnp.sum(weights, axis=3)
    vectors = jnp.einsum("nbcr,bre->nbce", weights, passages, precision=highest)
    highs, totals, vectors = reply((highs, totals, vectors))
    highs = highs.reshape(-1)[first_targets].reshape(-1, per_query)
    totals = totals.reshape(-1)[first_targets].reshape(-1, per_query)
    vectors = vectors.reshape(-1, embed_width)[first_targets].reshape(-1, per_query, embed_width)
    peak_high = jnp.max(highs, axis=1, keepdims=True)
    scaled = jnp.exp(highs - peak_high)
    denominator = jnp.sum(scaled * totals, axis=1)
    feedback = jnp.einsum("qk,qke->qe", scaled, vectors, precision=highest) / denominator[:, None]
    expanded = queries + coefficient * feedback
    expanded_sent = pack_rows(
        jnp.repeat(expanded, per_query, axis=0), second_targets, owners, resident_blocks, capacity
    )
    returned = (lambda arrived: send_back(project_onto_centroid(arrived)))(
        lax.all_to_all(expanded_sent, "cluster", split_axis=0, concat_axis=0, tiled=True)
    )
    second_scores = returned.reshape(-1, returned.shape[3])[second_targets].reshape(
        queries.shape[0], per_query, -1
    )
    return (expanded, second_scores)


def dot_nt(a, b):
    return lax.dot_general(a, b, (((1,), (1,)), ((), ())), preferred_element_type=jnp.float32)


def dot_nn(a, b):
    return lax.dot_general(a, b, (((1,), (0,)), ((), ())), preferred_element_type=jnp.float32)


def halves(x):
    high = x.astype(jnp.bfloat16)
    return high, (x - high.astype(jnp.float32)).astype(jnp.bfloat16)


def tools_of(corpus, turned_hi, turned_lo, pair, total, asked, names_of, part):
    both_rows = total.shape[0]
    top, _, size = asked.shape
    piece = size // 2
    lane = lax.broadcasted_iota(jnp.int32, (1, size), 1)

    def put_pair(x):
        high, low = halves(x)
        pair[pl.ds(0, x.shape[0]), :] = high
        pair[pl.ds(both_rows, x.shape[0]), :] = low

    def spread_out(held, wide, g):
        rows = held.shape[2]
        for j in range(top):
            line = held[g, j : j + 1, :].astype(jnp.float32)
            wide[j, pl.ds(g * rows, rows), :] = jnp.broadcast_to(line, (size, rows)).T

    def absorb(pieces, count, carry):
        peak, norm = carry
        group = pl.ds(0, count)
        highs, lows, names = [], [], []
        for unit, h in pieces:
            high, low = halves(
                jnp.concatenate([corpus[unit, 0, part(h), :], corpus[unit, 1, part(h), :]], axis=0)
            )
            place = pl.ds(h * size, size)
            turned_hi[unit, :, place] = high.T
            turned_lo[unit, :, place] = low.T
            highs.append(high)
            lows.append(low)
            own, others = names_of(unit)
            names.append(jnp.where(lane < piece, own, others))
        wide = [
            jnp.concatenate([turned[unit, :, pl.ds(h * size, size)] for unit, h in pieces], axis=1)
            for turned in (turned_hi, turned_lo)
        ]
        all_found = dot_three(
            pair[group, :], pair[pl.ds(both_rows, count), :], *wide
        )
        sums = [all_found[:, k * size : (k + 1) * size] for k in range(len(pieces))]
        parts, hits = [], []
        top_score = peak
        for name, found in zip(names, sums):
            hit = asked[0, group, :] == name
            for j in range(1, top):
                hit = jnp.logical_or(hit, asked[j, group, :] == name)
            score = jnp.where(hit, SOFTMAX_HEAT * found, MASKED)
            top_score = jnp.maximum(top_score, jnp.max(score, axis=1, keepdims=True))
            parts.append(score)
            hits.append(hit)
        shrink = jnp.exp(peak - top_score)
        weights = jnp.concatenate(
            [jnp.where(hit, jnp.exp(score - top_score), 0.0) for hit, score in zip(hits, parts)], axis=1
        )
        norm = norm * shrink + jnp.sum(weights, axis=1, keepdims=True)
        weight_high, weight_low = halves(weights)
        mixed = dot_three(
            weight_high, weight_low, jnp.concatenate(highs, axis=0), jnp.concatenate(lows, axis=0)
        )
        total[group, :] = total[group, :] * shrink + mixed
        return top_score, norm

    return put_pair, spread_out, absorb


def dot_three(high, low, right_high, right_low):
    return dot_nn(high, right_high) + (dot_nn(low, right_high) + dot_nn(high, right_low))


def nothing_yet(count):
    return jnp.full((count, 1), MASKED, jnp.float32), jnp.zeros((count, 1), jnp.float32)


def hub_kernel(
    queries_in, passages, first_in, followup_in, expanded, scores,
    first, followup, corpus, turned_hi, turned_lo, queries, pair, total, asked, chosen, picked,
    early, stats, scores_out,
    load_sem, send_c, recv_c, send_y, recv_y, send_z, recv_z, send_x, recv_x, send_back, recv_back,
):
    me = lax.axis_index("cluster")
    core, y, z = me % 2, (me // 2) % 2, me // 4
    rows, width = expanded.shape
    both_rows = 2 * rows
    top, _, size = asked.shape
    piece = size // 2
    inner = ((z + 1) % 4) // 2
    mate_z = z + 1 - 2 * (z % 2)
    hub_z = inner * z + (1 - inner) * mate_z
    end_z = inner * mate_z + (1 - inner) * z
    far_hub, far_end = 3 - hub_z, 3 - end_z

    def device(zz, yy, cc):
        return (2 * zz + yy) * 2 + cc

    mate = device(mate_z, y, core)
    beside = device(z, 1 - y, core)
    far = device(3 - z, y, core)
    other = device(z, y, 1 - core)

    plan = (
        (hub_z, y, 0), (hub_z, y, 1),
        (end_z, y, 0), (end_z, y, 1), (end_z, 1 - y, 1), (end_z, 1 - y, 0),
        (hub_z, 1 - y, 0), (hub_z, 1 - y, 1), (far_hub, 1 - y, 0), (far_hub, 1 - y, 1), (far_end, 1 - y, 0),
        (far_hub, y, 0), (far_hub, y, 1), (far_end, y, 0), (far_end, y, 1), (far_end, 1 - y, 1),
    )

    def names_of(unit):
        chip, index = 0, 0
        for k, (zz, yy, ii) in enumerate(plan):
            here = jnp.int32(unit == k) if isinstance(unit, int) else (unit == k).astype(jnp.int32)
            chip = chip + here * (2 * zz + yy)
            index = index + here * ii
        return (
            ((2 * chip + core) * 2 + index).astype(jnp.float32),
            ((2 * chip + 1 - core) * 2 + index).astype(jnp.float32),
        )

    def remote(src, dst, send, recv, target):
        return pltpu.make_async_remote_copy(
            src_ref=src, dst_ref=dst, send_sem=send, recv_sem=recv,
            device_id={"cluster": target}, device_id_type=pl.DeviceIdType.MESH,
        )

    def part(h):
        return pl.ds(h * piece, piece)

    def unit_copy(source, unit, sems, k, target):
        return remote(corpus.at[source, 0], corpus.at[unit, 0], sems[0].at[k], sems[1].at[k], target)

    def half_copy(source, unit, h, sems, k, target):
        return remote(
            corpus.at[source, 0, part(h)], corpus.at[unit, 0, part(h)],
            sems[0].at[k], sems[1].at[k], target,
        )

    on_c, on_y, on_z, on_x = (send_c, recv_c), (send_y, recv_y), (send_z, recv_z), (send_x, recv_x)

    def ids_up(k):
        held = (first, followup)[k]
        return remote(held.at[0], held.at[1], send_c.at[k], recv_c.at[k], mate)

    def queries_up():
        return remote(
            queries.at[pl.ds(0, rows)], queries.at[pl.ds(rows, rows)], send_c.at[2], recv_c.at[2], mate
        )

    def up(unit, h):
        source = unit - 2 if isinstance(unit, int) and unit < 4 else unit
        return half_copy(source, unit, h, on_c, 2 * unit + h, mate)

    def side(unit):
        return unit_copy(unit - 3 if isinstance(unit, int) and unit > 7 else unit, unit, on_y, unit, beside)

    def across(unit):
        return remote(corpus.at[unit, 0], corpus.at[unit, 1], send_x.at[unit], recv_x.at[unit], other)

    def across_half(unit, h):
        k = 16 + (unit // 5 - 1) * 2 + h
        return remote(
            corpus.at[unit, 0, part(h)], corpus.at[unit, 1, part(h)], send_x.at[k], recv_x.at[k], other
        )

    def back(k):
        source, target = (
            (early.at[0], early.at[1]),
            (stats.at[0], stats.at[1]),
            (scores_out, scores),
        )[k]
        return remote(source, target, send_back.at[k], recv_back.at[k], mate)

    def down(unit, h):
        k = 3 + 2 * (unit - 13) + h
        return half_copy(unit, unit, h, (send_back, recv_back), k, mate)

    loads = (
        pltpu.make_async_copy(passages.at[0], corpus.at[0, 0], load_sem.at[0]),
        pltpu.make_async_copy(passages.at[1], corpus.at[1, 0], load_sem.at[1]),
        pltpu.make_async_copy(queries_in, queries.at[pl.ds(0, rows)], load_sem.at[2]),
        pltpu.make_async_copy(first_in, first.at[0], load_sem.at[3]),
        pltpu.make_async_copy(followup_in, followup.at[0], load_sem.at[4]),
    )
    for load in loads:
        load.start()
    barrier = pltpu.get_barrier_semaphore()
    for target in (mate, beside, other):
        pl.semaphore_signal(
            barrier, inc=1, device_id={"cluster": target}, device_id_type=pl.DeviceIdType.MESH
        )

    @pl.when(inner == 1)
    def _():
        pl.semaphore_signal(
            barrier, inc=1, device_id={"cluster": far}, device_id_type=pl.DeviceIdType.MESH
        )

    pl.semaphore_wait(barrier, 3 + inner)
    for load in loads:
        load.wait()

    @pl.when(inner == 0)
    def _():
        ids_up(0).start()
        ids_up(1).start()
        queries_up().start()
        corner_side = [
            remote(corpus.at[k, 0], corpus.at[5 - k, 0], send_y.at[k], recv_y.at[k], beside)
            for k in (1, 0)
        ]
        for copy in corner_side:
            copy.start()
        for unit in (2, 3):
            for h in range(2):
                up(unit, h).start()
        put_pair, spread_out, absorb = tools_of(
            corpus, turned_hi, turned_lo, pair, total, asked, names_of, part
        )
        put_pair(queries[pl.ds(0, rows), :])
        spread_out(first, asked, 0)
        own = pl.ds(0, rows)
        total[own, :] = jnp.zeros((rows, width), jnp.float32)
        for copy, unit in zip(corner_side, (4, 5)):
            copy.wait_recv()
            for h in range(2):
                up(unit, h).start()
        for h in range(2):
            across_half(5, h).start()
        passed = [
            remote(
                corpus.at[source, 0, part(h)], corpus.at[unit, 0, part(h)],
                send_y.at[unit // 5 * 2 + h - 2], recv_y.at[unit // 5 * 2 + h - 2], beside,
            )
            for source, unit in ((13, 10), (14, 15))
            for h in range(2)
        ]

        def share(k):
            passed[k].wait_recv()
            across_half(10 + k // 2 * 5, k % 2).start()

        for k in range(4):
            down(13 + k // 2, k % 2).wait_recv()
            passed[k].start()
            if k > 0:
                share(k - 1)
        share(3)

        def late(h, carry):
            for unit in (5, 10, 15):
                across_half(unit, h).wait_recv()
            return absorb([(5, h), (10, h), (15, h)], rows, carry)

        peak, norm = lax.fori_loop(0, 2, late, nothing_yet(rows))
        for k in range(2):
            back(k).wait_recv()
        early_peak, early_norm = (
            jnp.broadcast_to(stats[1, k, 0:1, :], (size, rows)).T[:, 0:1] for k in range(2)
        )
        top_score = jnp.maximum(peak, early_peak)
        shrink, early_shrink = jnp.exp(peak - top_score), jnp.exp(early_peak - top_score)
        norm = norm * shrink + early_norm * early_shrink
        mixed = total[own, :] * shrink + early[1] * early_shrink
        expanded[...] = queries[own, :] + (FEEDBACK * width ** (-0.5)) * (mixed / norm)
        back(2).wait_recv()
        for copy in passed:
            copy.wait_send()
        for unit in (5, 10, 15):
            for h in range(2):
                across_half(unit, h).wait_send()
        ids_up(0).wait_send()
        ids_up(1).wait_send()
        queries_up().wait_send()
        for copy in corner_side:
            copy.wait_send()
        for unit in (2, 3, 4, 5):
            for h in range(2):
                up(unit, h).wait_send()

    @pl.when(inner == 1)
    def _():
        hub(
            first, followup, corpus, turned_hi, turned_lo, queries, pair, total, asked, chosen,
            picked, expanded, scores, early, stats, scores_out,
            names_of, unit_copy, half_copy, ids_up, queries_up, across, across_half, back, down, part,
            on_c, on_y, on_z, mate, beside, far,
        )


def hub(
    first, followup, corpus, turned_hi, turned_lo, queries, pair, total, asked, chosen,
    picked, expanded, scores, early, stats, scores_out,
    names_of, unit_copy, half_copy, ids_up, queries_up, across, across_half, back, down, part,
    on_c, on_y, on_z, mate, beside, far,
):
    rows, width = expanded.shape
    both_rows = 2 * rows
    top, _, size = asked.shape
    piece = size // 2
    lane = lax.broadcasted_iota(jnp.int32, (1, size), 1)

    def from_mate(unit, h):
        return half_copy(unit, unit, h, on_c, 2 * unit + h, mate)

    def from_side(t):
        return unit_copy(5 + t, 5 + t, on_y, 5 + t, beside)

    def last_side(h):
        return half_copy(13, 10, h, on_y, 10 + h, beside)

    def own_side(k):
        return unit_copy(k, 6 + k, on_y, 6 + k, beside)

    def pass_side(t):
        return unit_copy(10 + t, 7 + t, on_y, 7 + t, beside)

    def own_far(k):
        return unit_copy(k, 11 + k, on_z, k, far)

    def pass_far(t, h):
        return half_copy(t, 11 + t, h, on_z, 2 * t + h, far)

    def from_far(t):
        return unit_copy(10 + t, 10 + t, on_z, t - 1, far)

    def from_far_half(t, h):
        return half_copy(10 + t, 10 + t, h, on_z, 2 * (t - 1) + h, far)

    for k in range(2):
        own_far(k).start()
        own_side(k).start()
    for k in range(2):
        across(k).start()
    from_far(1).wait_recv()
    pass_side(1).start()
    across(11).start()
    from_side(1).wait_recv()
    across(6).start()
    for k in range(2):
        ids_up(k).wait_recv()
    queries_up().wait_recv()

    put_pair, spread_out, absorb = tools_of(
        corpus, turned_hi, turned_lo, pair, total, asked, names_of, part
    )
    put_pair(queries[...])
    total[...] = jnp.zeros_like(total)
    picked[...] = jnp.zeros_like(picked)
    for g in range(2):
        spread_out(first, asked, g)
        spread_out(followup, chosen, g)

    def take(unit, carry):
        across(unit).wait_recv()
        return absorb([(unit, 0), (unit, 1)], both_rows, carry)

    def step(t, carry):
        carry = take(4 + t, carry)
        carry = take(t - 1, carry)

        @pl.when(t < 5)
        def _():
            from_mate(t, 0).wait_recv()
            pass_far(t, 0).start()

            @pl.when(t > 2)
            def _():
                from_far_half(t, 0).wait_recv()
                down(10 + t, 0).start()

        carry = take(9 + t, carry)

        @pl.when(t < 5)
        def _():
            from_mate(t, 1).wait_recv()
            pass_far(t, 1).start()
            across(t).start()

            @pl.when(t == 2)
            def _():
                from_far(t).wait_recv()
                pass_side(t).start()

            @pl.when(t > 2)
            def _():
                from_far_half(t, 1).wait_recv()
                down(10 + t, 1).start()

            across(10 + t).start()
            from_side(t).wait_recv()
            across(5 + t).start()

            @pl.when(t == 3)
            def _():
                for h in range(2):
                    last_side(h).start()

        return carry

    carry = nothing_yet(both_rows)
    carry = take(0, carry)
    carry = lax.fori_loop(2, 6, step, carry)

    early[0] = total[pl.ds(rows, rows), :]
    for k in range(2):
        line = jnp.broadcast_to(carry[k][rows:], (rows, size)).T
        stats[0, k] = line[: stats.shape[2], :]
    back(1).start()
    back(0).start()

    def finish(h, carry):
        from_mate(5, h).wait_recv()
        across_half(5, h).start()
        last_side(h).wait_recv()
        across_half(10, h).start()
        from_far_half(5, h).wait_recv()
        across_half(15, h).start()
        for unit in (5, 10, 15):
            across_half(unit, h).wait_recv()
        return absorb([(5, h), (10, h), (15, h)], both_rows, carry)

    _, norm = lax.fori_loop(0, 2, finish, carry)

    after = queries[...] + (FEEDBACK * width ** (-0.5)) * (total[...] / norm)
    put_pair(after)
    expanded[...] = after[:rows]

    def score_all(g, out):
        group = pl.ds(g * rows, rows)

        def second_round(turn, carry):
            values = [picked[j, group, :] for j in range(top)]
            for k in range(4):
                unit = 4 * turn + k
                found = dot_three(
                    pair[group, :], pair[pl.ds(both_rows + g * rows, rows), :],
                    turned_hi[unit], turned_lo[unit],
                )
                a, b = found[:, :size], found[:, size:]
                own = jnp.where(lane < piece, a, pltpu.roll(b, piece, 1))
                others = jnp.where(lane < piece, pltpu.roll(a, piece, 1), b)
                names = names_of(unit)
                for j in range(top):
                    value = jnp.where(chosen[j, group, :] == names[0], own, values[j])
                    values[j] = jnp.where(chosen[j, group, :] == names[1], others, value)
            for j in range(top):
                picked[j, group, :] = values[j]
            return carry

        lax.fori_loop(0, 4, second_round, 0)
        for j in range(top):
            out[:, j, :] = picked[j, group, :]

    score_all(1, scores_out)
    back(2).start()
    score_all(0, scores)

    for k in range(2):
        own_far(k).wait_send()
        own_side(k).wait_send()
        pass_side(1 + k).wait_send()
        last_side(k).wait_send()
    for k in range(3):
        back(k).wait_send()
    for unit in (13, 14):
        for h in range(2):
            down(unit, h).wait_send()

    def drain(t, carry):
        for h in range(2):
            pass_far(t, h).wait_send()
        return carry

    lax.fori_loop(2, 5, drain, 0)

    def drain_across(unit, carry):
        @pl.when(unit % 5 != 0)
        def _():
            across(unit).wait_send()

        return carry

    across(0).wait_send()
    lax.fori_loop(1, 15, drain_across, 0)
    for unit in (5, 10, 15):
        for h in range(2):
            across_half(unit, h).wait_send()


def grant_of(queries, passages, first_blocks):
    resident, size, width = passages.shape
    rows = queries.shape[0]
    corpus = lax.axis_size("cluster") * resident * size * width * 8
    return corpus + (12 * rows * width + 10 * first_blocks.shape[1] * rows * size) * 4


def hub_fits(queries, passages, first_blocks):
    owners = lax.axis_size("cluster")
    resident, size, _ = passages.shape
    fits = grant_of(queries, passages, first_blocks) < VMEM_BYTES
    return owners == 16 and resident == 2 and fits and queries.shape[0] == size


def device_program(queries, passages, first_blocks, followup_blocks):
    if not hub_fits(queries, passages, first_blocks):
        return local(queries, passages, first_blocks, followup_blocks)
    units = lax.axis_size("cluster")
    rows, width = queries.shape
    size = passages.shape[1]
    top = first_blocks.shape[1]
    vmem = pl.BlockSpec(memory_space=pltpu.VMEM)
    hbm = pl.BlockSpec(memory_space=pltpu.HBM)
    operands = (queries, passages, first_blocks.T, followup_blocks.T)
    dma = pltpu.SemaphoreType.DMA
    return pl.pallas_call(
        hub_kernel,
        out_shape=(
            jax.ShapeDtypeStruct((rows, width), jnp.float32),
            jax.ShapeDtypeStruct((rows, top, size), jnp.float32),
        ),
        in_specs=[hbm, hbm, hbm, hbm],
        out_specs=(vmem, vmem),
        scratch_shapes=[
            pltpu.VMEM((2, top, rows), jnp.int32),
            pltpu.VMEM((2, top, rows), jnp.int32),
            pltpu.VMEM((units, 2, size, width), jnp.float32),
            pltpu.VMEM((units, width, 2 * size), jnp.bfloat16),
            pltpu.VMEM((units, width, 2 * size), jnp.bfloat16),
            pltpu.VMEM((2 * rows, width), jnp.float32),
            pltpu.VMEM((4 * rows, width), jnp.bfloat16),
            pltpu.VMEM((2 * rows, width), jnp.float32),
            pltpu.VMEM((top, 2 * rows, size), jnp.float32),
            pltpu.VMEM((top, 2 * rows, size), jnp.float32),
            pltpu.VMEM((top, 2 * rows, size), jnp.float32),
            pltpu.VMEM((2, rows, width), jnp.float32),
            pltpu.VMEM((2, 2, 8, rows), jnp.float32),
            pltpu.VMEM((rows, top, size), jnp.float32),
            dma((5,)),
            dma((12,)), dma((12,)),
            dma((12,)), dma((12,)),
            dma((10,)), dma((10,)),
            dma((22,)), dma((22,)),
            dma((7,)), dma((7,)),
        ],
        compiler_params=pltpu.CompilerParams(
            collective_id=0, has_side_effects=True, vmem_limit_bytes=VMEM_BYTES
        ),
    )(*[pltpu.with_memory_space_constraint(x, pltpu.HBM) for x in operands])


def solution(mesh):
    return jax.shard_map(
        device_program,
        mesh=mesh,
        in_specs=(
            P(("parts", "cluster"), None),
            P(("parts", "cluster"), None, None),
            P(("parts", "cluster"), None),
            P(("parts", "cluster"), None),
        ),
        out_specs=(P(("parts", "cluster"), None), P(("parts", "cluster"), None, None)),
        check_vma=False,
    )
```

```python
import functools

import jax
import jax.numpy as jnp
from jax import lax
from jax.experimental import pallas as pl
from jax.experimental.pallas import tpu as pltpu
from jax.sharding import PartitionSpec as P

SOFTMAX_HEAT = 2.0
FEEDBACK = 0.5
MASKED = -1e30
VMEM_BYTES = 50 * 1024 * 1024


def position_targets(block_ids, capacity):
    flat_ids = block_ids.reshape(-1)
    matches = flat_ids[:, None] == flat_ids[None, :]
    positions = jnp.arange(flat_ids.shape[0], dtype=jnp.int32)
    earlier = positions[None, :] < positions[:, None]
    ranking = jnp.sum(jnp.logical_and(matches, earlier), axis=1, dtype=jnp.int32)
    return flat_ids * capacity + ranking


def pack_rows(values, targets, owners, resident_blocks, capacity):
    buffer = jnp.zeros((owners * resident_blocks * capacity, values.shape[1]), values.dtype)
    buffer = buffer.at[targets].set(values)
    return buffer.reshape(owners, resident_blocks, capacity, values.shape[1])


def reply(results):
    return (
        lax.all_to_all(results[0], "cluster", split_axis=0, concat_axis=0, tiled=True),
        lax.all_to_all(results[1], "cluster", split_axis=0, concat_axis=0, tiled=True),
        lax.all_to_all(results[2], "cluster", split_axis=0, concat_axis=0, tiled=True),
    )


def send_back(match_scores):
    return lax.all_to_all(match_scores, "cluster", split_axis=0, concat_axis=0, tiled=True)


def local(queries, passages, first_blocks, followup_blocks):
    owners = lax.axis_size("cluster")
    resident_blocks = passages.shape[0]
    embed_width = queries.shape[1]
    per_query = first_blocks.shape[1]
    pair_count = queries.shape[0] * per_query
    all_blocks = owners * resident_blocks
    capacity = max(2, (3 * pair_count + 2 * all_blocks - 1) // (2 * all_blocks))
    coefficient = FEEDBACK * embed_width ** (-0.5)
    highest = lax.Precision.HIGHEST

    def project_onto_centroid(arrived):
        return jnp.einsum("nbce,bre->nbcr", arrived, passages, precision=highest)

    first_targets = position_targets(first_blocks, capacity)
    second_targets = position_targets(followup_blocks, capacity)
    repeated = jnp.repeat(queries, per_query, axis=0)
    first_sent = pack_rows(repeated, first_targets, owners, resident_blocks, capacity)
    match_scores = SOFTMAX_HEAT * project_onto_centroid(
        lax.all_to_all(first_sent, "cluster", split_axis=0, concat_axis=0, tiled=True)
    )
    highs = jnp.max(match_scores, axis=3)
    weights = jnp.exp(match_scores - highs[..., None])
    totals = jnp.sum(weights, axis=3)
    vectors = jnp.einsum("nbcr,bre->nbce", weights, passages, precision=highest)
    highs, totals, vectors = reply((highs, totals, vectors))
    highs = highs.reshape(-1)[first_targets].reshape(-1, per_query)
    totals = totals.reshape(-1)[first_targets].reshape(-1, per_query)
    vectors = vectors.reshape(-1, embed_width)[first_targets].reshape(-1, per_query, embed_width)
    peak_high = jnp.max(highs, axis=1, keepdims=True)
    scaled = jnp.exp(highs - peak_high)
    denominator = jnp.sum(scaled * totals, axis=1)
    feedback = jnp.einsum("qk,qke->qe", scaled, vectors, precision=highest) / denominator[:, None]
    expanded = queries + coefficient * feedback
    expanded_sent = pack_rows(
        jnp.repeat(expanded, per_query, axis=0), second_targets, owners, resident_blocks, capacity
    )
    returned = (lambda arrived: send_back(project_onto_centroid(arrived)))(
        lax.all_to_all(expanded_sent, "cluster", split_axis=0, concat_axis=0, tiled=True)
    )
    second_scores = returned.reshape(-1, returned.shape[3])[second_targets].reshape(
        queries.shape[0], per_query, -1
    )
    return (expanded, second_scores)


def dot_nt(a, b):
    return lax.dot_general(a, b, (((1,), (1,)), ((), ())), preferred_element_type=jnp.float32)


def dot_nn(a, b):
    return lax.dot_general(a, b, (((1,), (0,)), ((), ())), preferred_element_type=jnp.float32)


def halves(x):
    high = x.astype(jnp.bfloat16)
    return high, (x - high.astype(jnp.float32)).astype(jnp.bfloat16)


def tools_of(
    corpus, turned_hi, turned_lo, pair, total, asked, chosen, picked, names_of, part
):
    both_rows = total.shape[0]
    top, _, size = asked.shape
    piece = size // 2
    lane = lax.broadcasted_iota(jnp.int32, (1, size), 1)

    def put_pair(x):
        high, low = halves(x)
        pair[pl.ds(0, x.shape[0]), :] = high
        pair[pl.ds(both_rows, x.shape[0]), :] = low

    def spread_out(held, wide, g):
        rows = held.shape[2]
        for j in range(top):
            line = held[g, j : j + 1, :].astype(jnp.float32)
            wide[j, pl.ds(g * rows, rows), :] = jnp.broadcast_to(line, (size, rows)).T

    def absorb(pieces, count, carry):
        peak, norm = carry
        group = pl.ds(0, count)
        highs, lows, names = [], [], []
        for unit, h in pieces:
            high, low = turn_over(unit, unit, h)
            highs.append(high)
            lows.append(low)
            own, others = names_of(unit)
            names.append(jnp.where(lane < piece, own, others))
        wide = [
            jnp.concatenate([turned[unit, :, pl.ds(h * size, size)] for unit, h in pieces], axis=1)
            for turned in (turned_hi, turned_lo)
        ]
        all_found = dot_three(
            pair[group, :], pair[pl.ds(both_rows, count), :], *wide
        )
        sums = [all_found[:, k * size : (k + 1) * size] for k in range(len(pieces))]
        parts, hits = [], []
        top_score = peak
        for name, found in zip(names, sums):
            hit = asked[0, group, :] == name
            for j in range(1, top):
                hit = jnp.logical_or(hit, asked[j, group, :] == name)
            score = jnp.where(hit, SOFTMAX_HEAT * found, MASKED)
            top_score = jnp.maximum(top_score, jnp.max(score, axis=1, keepdims=True))
            parts.append(score)
            hits.append(hit)
        shrink = jnp.exp(peak - top_score)
        weights = jnp.concatenate(
            [jnp.where(hit, jnp.exp(score - top_score), 0.0) for hit, score in zip(hits, parts)], axis=1
        )
        norm = norm * shrink + jnp.sum(weights, axis=1, keepdims=True)
        weight_high, weight_low = halves(weights)
        mixed = dot_three(
            weight_high, weight_low, jnp.concatenate(highs, axis=0), jnp.concatenate(lows, axis=0)
        )
        total[group, :] = total[group, :] * shrink + mixed
        return top_score, norm

    def turn_over(source, unit, h):
        high, low = halves(
            jnp.concatenate([corpus[source, 0, part(h), :], corpus[source, 1, part(h), :]], axis=0)
        )
        place = pl.ds(h * size, size)
        turned_hi[unit, :, place] = high.T
        turned_lo[unit, :, place] = low.T
        return high, low

    def score_units(g, rows, turns, starts, strides):
        group = pl.ds(g * rows, rows)

        def second_round(turn, carry):
            values = [picked[j, group, :] for j in range(top)]
            for start, stride in zip(starts, strides):
                unit = start + stride * turn
                found = dot_three(
                    pair[group, :], pair[pl.ds(both_rows + g * rows, rows), :],
                    turned_hi[unit], turned_lo[unit],
                )
                a, b = found[:, :size], found[:, size:]
                own = jnp.where(lane < piece, a, pltpu.roll(b, piece, 1))
                others = jnp.where(lane < piece, pltpu.roll(a, piece, 1), b)
                names = names_of(unit)
                for j in range(top):
                    value = jnp.where(chosen[j, group, :] == names[0], own, values[j])
                    values[j] = jnp.where(chosen[j, group, :] == names[1], others, value)
            for j in range(top):
                picked[j, group, :] = values[j]
            return carry

        lax.fori_loop(0, turns, second_round, 0)

    return put_pair, spread_out, absorb, turn_over, score_units


def dot_three(high, low, right_high, right_low):
    return dot_nn(high, right_high) + (dot_nn(low, right_high) + dot_nn(high, right_low))


def nothing_yet(count):
    return jnp.full((count, 1), MASKED, jnp.float32), jnp.zeros((count, 1), jnp.float32)


def hub_kernel(
    queries_in, passages, first_in, followup_in, expanded, scores,
    first, followup, corpus, turned_hi, turned_lo, queries, pair, total, asked, chosen, picked,
    early, stats, scores_out,
    load_sem, send_c, recv_c, send_y, recv_y, send_z, recv_z, send_x, recv_x, send_back, recv_back,
):
    me = lax.axis_index("cluster")
    core, y, z = me % 2, (me // 2) % 2, me // 4
    rows, width = expanded.shape
    both_rows = 2 * rows
    top, _, size = asked.shape
    piece = size // 2
    inner = ((z + 1) % 4) // 2
    mate_z = z + 1 - 2 * (z % 2)
    hub_z = inner * z + (1 - inner) * mate_z
    end_z = inner * mate_z + (1 - inner) * z
    far_hub, far_end = 3 - hub_z, 3 - end_z

    def device(zz, yy, cc):
        return (2 * zz + yy) * 2 + cc

    mate = device(mate_z, y, core)
    beside = device(z, 1 - y, core)
    far = device(3 - z, y, core)
    other = device(z, y, 1 - core)

    plan = (
        (hub_z, y, 0), (hub_z, y, 1),
        (end_z, y, 0), (end_z, y, 1), (end_z, 1 - y, 1), (end_z, 1 - y, 0),
        (hub_z, 1 - y, 0), (hub_z, 1 - y, 1), (far_hub, 1 - y, 0), (far_hub, 1 - y, 1), (far_end, 1 - y, 0),
        (far_hub, y, 0), (far_hub, y, 1), (far_end, y, 0), (far_end, y, 1), (far_end, 1 - y, 1),
    )

    def names_of(unit):
        chip, index = 0, 0
        for k, (zz, yy, ii) in enumerate(plan):
            here = jnp.int32(unit == k) if isinstance(unit, int) else (unit == k).astype(jnp.int32)
            chip = chip + here * (2 * zz + yy)
            index = index + here * ii
        return (
            ((2 * chip + core) * 2 + index).astype(jnp.float32),
            ((2 * chip + 1 - core) * 2 + index).astype(jnp.float32),
        )

    def remote(src, dst, send, recv, target):
        return pltpu.make_async_remote_copy(
            src_ref=src, dst_ref=dst, send_sem=send, recv_sem=recv,
            device_id={"cluster": target}, device_id_type=pl.DeviceIdType.MESH,
        )

    def part(h):
        return pl.ds(h * piece, piece)

    def unit_copy(source, unit, sems, k, target):
        return remote(corpus.at[source, 0], corpus.at[unit, 0], sems[0].at[k], sems[1].at[k], target)

    def half_copy(source, unit, h, sems, k, target):
        return remote(
            corpus.at[source, 0, part(h)], corpus.at[unit, 0, part(h)],
            sems[0].at[k], sems[1].at[k], target,
        )

    on_c, on_y, on_z, on_x = (send_c, recv_c), (send_y, recv_y), (send_z, recv_z), (send_x, recv_x)

    def ids_up(k):
        held = (first, followup)[k]
        return remote(held.at[0], held.at[1], send_c.at[k], recv_c.at[k], mate)

    def queries_up():
        return remote(
            queries.at[pl.ds(0, rows)], queries.at[pl.ds(rows, rows)], send_c.at[2], recv_c.at[2], mate
        )

    def up(unit, h):
        source = unit - 2 if isinstance(unit, int) and unit < 4 else unit
        return half_copy(source, unit, h, on_c, 2 * unit + h, mate)

    def side(unit):
        return unit_copy(unit - 3 if isinstance(unit, int) and unit > 7 else unit, unit, on_y, unit, beside)

    def across(unit):
        return remote(corpus.at[unit, 0], corpus.at[unit, 1], send_x.at[unit], recv_x.at[unit], other)

    def across_half(unit, h):
        k = 16 + (unit // 5 - 1) * 2 + h
        return remote(
            corpus.at[unit, 0, part(h)], corpus.at[unit, 1, part(h)], send_x.at[k], recv_x.at[k], other
        )

    def back(k):
        source, target = (
            (early.at[0], early.at[1]),
            (stats.at[0], stats.at[1]),
            (scores_out, scores),
        )[k]
        return remote(source, target, send_back.at[k], recv_back.at[k], mate)

    def down(unit, h):
        k = 3 + 2 * (unit - 13) + h
        return half_copy(unit, unit, h, (send_back, recv_back), k, mate)

    loads = (
        pltpu.make_async_copy(passages.at[0], corpus.at[0, 0], load_sem.at[0]),
        pltpu.make_async_copy(passages.at[1], corpus.at[1, 0], load_sem.at[1]),
        pltpu.make_async_copy(queries_in, queries.at[pl.ds(0, rows)], load_sem.at[2]),
        pltpu.make_async_copy(first_in, first.at[0], load_sem.at[3]),
        pltpu.make_async_copy(followup_in, followup.at[0], load_sem.at[4]),
    )
    for load in loads:
        load.start()
    barrier = pltpu.get_barrier_semaphore()
    for target in (mate, beside, other):
        pl.semaphore_signal(
            barrier, inc=1, device_id={"cluster": target}, device_id_type=pl.DeviceIdType.MESH
        )

    @pl.when(inner == 1)
    def _():
        pl.semaphore_signal(
            barrier, inc=1, device_id={"cluster": far}, device_id_type=pl.DeviceIdType.MESH
        )

    pl.semaphore_wait(barrier, 3 + inner)
    for load in loads:
        load.wait()

    @pl.when(inner == 0)
    def _():
        ids_up(0).start()
        ids_up(1).start()
        queries_up().start()
        corner_side = [
            remote(corpus.at[k, 0], corpus.at[5 - k, 0], send_y.at[k], recv_y.at[k], beside)
            for k in (1, 0)
        ]
        for copy in corner_side:
            copy.start()
        for unit in (2, 3):
            for h in range(2):
                up(unit, h).start()
        put_pair, spread_out, absorb, turn_over, score_units = tools_of(
            corpus, turned_hi, turned_lo, pair, total, asked, chosen, picked, names_of, part
        )
        put_pair(queries[pl.ds(0, rows), :])
        spread_out(first, asked, 0)
        spread_out(followup, chosen, 0)
        own = pl.ds(0, rows)
        for k in range(2):
            across(k).start()
        for j in range(top):
            picked[j, own, :] = jnp.zeros((rows, size), jnp.float32)
        total[own, :] = jnp.zeros((rows, width), jnp.float32)
        for copy, unit in zip(corner_side, (4, 5)):
            copy.wait_recv()
            for h in range(2):
                up(unit, h).start()
        for h in range(2):
            across_half(5, h).start()
        across(4).start()
        for source, unit in ((0, 2), (1, 3), (4, 4)):
            across(source).wait_recv()
            for h in range(2):
                turn_over(source, unit, h)
        passed = [
            remote(
                corpus.at[source, 0, part(h)], corpus.at[unit, 0, part(h)],
                send_y.at[unit // 5 * 2 + h - 2], recv_y.at[unit // 5 * 2 + h - 2], beside,
            )
            for source, unit in ((13, 10), (14, 15))
            for h in range(2)
        ]

        def share(k):
            passed[k].wait_recv()
            across_half(10 + k // 2 * 5, k % 2).start()

        for k in range(4):
            down(13 + k // 2, k % 2).wait_recv()
            passed[k].start()
            if k % 2 == 1:
                across(13 + k // 2).start()
            if k > 0:
                share(k - 1)
        share(3)

        def late(h, carry):
            for unit in (5, 10, 15):
                across_half(unit, h).wait_recv()
            return absorb([(5, h), (10, h), (15, h)], rows, carry)

        peak, norm = lax.fori_loop(0, 2, late, nothing_yet(rows))
        for unit in (13, 14):
            across(unit).wait_recv()
            for h in range(2):
                turn_over(unit, unit, h)
        for k in range(2):
            back(k).wait_recv()
        early_peak, early_norm = (
            jnp.broadcast_to(stats[1, k, 0:1, :], (size, rows)).T[:, 0:1] for k in range(2)
        )
        top_score = jnp.maximum(peak, early_peak)
        shrink, early_shrink = jnp.exp(peak - top_score), jnp.exp(early_peak - top_score)
        norm = norm * shrink + early_norm * early_shrink
        mixed = total[own, :] * shrink + early[1] * early_shrink
        after = queries[own, :] + (FEEDBACK * width ** (-0.5)) * (mixed / norm)
        expanded[...] = after
        put_pair(after)
        score_units(0, rows, 2, (2, 3, 4, 5), (8, 10, 10, 10))
        back(2).wait_recv()
        for j in range(top):
            scores[:, j, :] = scores[:, j, :] + picked[j, own, :]
        for unit in (0, 1, 4, 13, 14):
            across(unit).wait_send()
        for copy in passed:
            copy.wait_send()
        for unit in (5, 10, 15):
            for h in range(2):
                across_half(unit, h).wait_send()
        ids_up(0).wait_send()
        ids_up(1).wait_send()
        queries_up().wait_send()
        for copy in corner_side:
            copy.wait_send()
        for unit in (2, 3, 4, 5):
            for h in range(2):
                up(unit, h).wait_send()

    @pl.when(inner == 1)
    def _():
        hub(
            first, followup, corpus, turned_hi, turned_lo, queries, pair, total, asked, chosen,
            picked, expanded, scores, early, stats, scores_out,
            names_of, unit_copy, half_copy, ids_up, queries_up, across, across_half, back, down, part,
            on_c, on_y, on_z, mate, beside, far,
        )


def hub(
    first, followup, corpus, turned_hi, turned_lo, queries, pair, total, asked, chosen,
    picked, expanded, scores, early, stats, scores_out,
    names_of, unit_copy, half_copy, ids_up, queries_up, across, across_half, back, down, part,
    on_c, on_y, on_z, mate, beside, far,
):
    rows, width = expanded.shape
    both_rows = 2 * rows
    top, _, size = asked.shape
    piece = size // 2
    lane = lax.broadcasted_iota(jnp.int32, (1, size), 1)

    def from_mate(unit, h):
        return half_copy(unit, unit, h, on_c, 2 * unit + h, mate)

    def from_side(t):
        return unit_copy(5 + t, 5 + t, on_y, 5 + t, beside)

    def last_side(h):
        return half_copy(13, 10, h, on_y, 10 + h, beside)

    def own_side(k):
        return unit_copy(k, 6 + k, on_y, 6 + k, beside)

    def pass_side(t):
        return unit_copy(10 + t, 7 + t, on_y, 7 + t, beside)

    def own_far(k):
        return unit_copy(k, 11 + k, on_z, k, far)

    def pass_far(t, h):
        return half_copy(t, 11 + t, h, on_z, 2 * t + h, far)

    def from_far(t):
        return unit_copy(10 + t, 10 + t, on_z, t - 1, far)

    def from_far_half(t, h):
        return half_copy(10 + t, 10 + t, h, on_z, 2 * (t - 1) + h, far)

    for k in range(2):
        own_far(k).start()
        own_side(k).start()
    for k in range(2):
        across(k).start()
    from_far(1).wait_recv()
    pass_side(1).start()
    across(11).start()
    from_side(1).wait_recv()
    across(6).start()
    for k in range(2):
        ids_up(k).wait_recv()
    queries_up().wait_recv()

    put_pair, spread_out, absorb, turn_over, score_units = tools_of(
        corpus, turned_hi, turned_lo, pair, total, asked, chosen, picked, names_of, part
    )
    put_pair(queries[...])
    total[...] = jnp.zeros_like(total)
    picked[...] = jnp.zeros_like(picked)
    for g in range(2):
        spread_out(first, asked, g)
        spread_out(followup, chosen, g)

    def take(unit, carry):
        across(unit).wait_recv()
        return absorb([(unit, 0), (unit, 1)], both_rows, carry)

    def step(t, carry):
        carry = take(4 + t, carry)
        carry = take(t - 1, carry)

        @pl.when(t < 5)
        def _():
            from_mate(t, 0).wait_recv()
            pass_far(t, 0).start()

            @pl.when(t > 2)
            def _():
                from_far_half(t, 0).wait_recv()
                down(10 + t, 0).start()

        carry = take(9 + t, carry)

        @pl.when(t < 5)
        def _():
            from_mate(t, 1).wait_recv()
            pass_far(t, 1).start()
            across(t).start()

            @pl.when(t == 2)
            def _():
                from_far(t).wait_recv()
                pass_side(t).start()

            @pl.when(t > 2)
            def _():
                from_far_half(t, 1).wait_recv()
                down(10 + t, 1).start()

            across(10 + t).start()
            from_side(t).wait_recv()
            across(5 + t).start()

            @pl.when(t == 3)
            def _():
                for h in range(2):
                    last_side(h).start()

        return carry

    carry = nothing_yet(both_rows)
    carry = take(0, carry)
    carry = lax.fori_loop(2, 6, step, carry)

    early[0] = total[pl.ds(rows, rows), :]
    for k in range(2):
        line = jnp.broadcast_to(carry[k][rows:], (rows, size)).T
        stats[0, k] = line[: stats.shape[2], :]
    back(1).start()
    back(0).start()

    def finish(h, carry):
        from_mate(5, h).wait_recv()
        across_half(5, h).start()
        last_side(h).wait_recv()
        across_half(10, h).start()
        from_far_half(5, h).wait_recv()
        across_half(15, h).start()
        for unit in (5, 10, 15):
            across_half(unit, h).wait_recv()
        return absorb([(5, h), (10, h), (15, h)], both_rows, carry)

    _, norm = lax.fori_loop(0, 2, finish, carry)

    after = queries[...] + (FEEDBACK * width ** (-0.5)) * (total[...] / norm)
    put_pair(after)
    expanded[...] = after[:rows]

    score_units(1, rows, 2, (0, 1, 6, 7), (8, 8, 5, 5))
    for j in range(top):
        scores_out[:, j, :] = picked[j, pl.ds(rows, rows), :]
    back(2).start()
    score_units(0, rows, 4, (0, 1, 2, 3), (4, 4, 4, 4))
    for j in range(top):
        scores[:, j, :] = picked[j, pl.ds(0, rows), :]

    for k in range(2):
        own_far(k).wait_send()
        own_side(k).wait_send()
        pass_side(1 + k).wait_send()
        last_side(k).wait_send()
    for k in range(3):
        back(k).wait_send()
    for unit in (13, 14):
        for h in range(2):
            down(unit, h).wait_send()

    def drain(t, carry):
        for h in range(2):
            pass_far(t, h).wait_send()
        return carry

    lax.fori_loop(2, 5, drain, 0)

    def drain_across(unit, carry):
        @pl.when(unit % 5 != 0)
        def _():
            across(unit).wait_send()

        return carry

    across(0).wait_send()
    lax.fori_loop(1, 15, drain_across, 0)
    for unit in (5, 10, 15):
        for h in range(2):
            across_half(unit, h).wait_send()


def grant_of(queries, passages, first_blocks):
    resident, size, width = passages.shape
    rows = queries.shape[0]
    corpus = lax.axis_size("cluster") * resident * size * width * 8
    return corpus + (12 * rows * width + 10 * first_blocks.shape[1] * rows * size) * 4


def hub_fits(queries, passages, first_blocks):
    owners = lax.axis_size("cluster")
    resident, size, _ = passages.shape
    fits = grant_of(queries, passages, first_blocks) < VMEM_BYTES
    return owners == 16 and resident == 2 and fits and queries.shape[0] == size


def device_program(queries, passages, first_blocks, followup_blocks):
    if not hub_fits(queries, passages, first_blocks):
        return local(queries, passages, first_blocks, followup_blocks)
    units = lax.axis_size("cluster")
    rows, width = queries.shape
    size = passages.shape[1]
    top = first_blocks.shape[1]
    vmem = pl.BlockSpec(memory_space=pltpu.VMEM)
    hbm = pl.BlockSpec(memory_space=pltpu.HBM)
    operands = (queries, passages, first_blocks.T, followup_blocks.T)
    dma = pltpu.SemaphoreType.DMA
    return pl.pallas_call(
        hub_kernel,
        out_shape=(
            jax.ShapeDtypeStruct((rows, width), jnp.float32),
            jax.ShapeDtypeStruct((rows, top, size), jnp.float32),
        ),
        in_specs=[hbm, hbm, hbm, hbm],
        out_specs=(vmem, vmem),
        scratch_shapes=[
            pltpu.VMEM((2, top, rows), jnp.int32),
            pltpu.VMEM((2, top, rows), jnp.int32),
            pltpu.VMEM((units, 2, size, width), jnp.float32),
            pltpu.VMEM((units, width, 2 * size), jnp.bfloat16),
            pltpu.VMEM((units, width, 2 * size), jnp.bfloat16),
            pltpu.VMEM((2 * rows, width), jnp.float32),
            pltpu.VMEM((4 * rows, width), jnp.bfloat16),
            pltpu.VMEM((2 * rows, width), jnp.float32),
            pltpu.VMEM((top, 2 * rows, size), jnp.float32),
            pltpu.VMEM((top, 2 * rows, size), jnp.float32),
            pltpu.VMEM((top, 2 * rows, size), jnp.float32),
            pltpu.VMEM((2, rows, width), jnp.float32),
            pltpu.VMEM((2, 2, 8, rows), jnp.float32),
            pltpu.VMEM((rows, top, size), jnp.float32),
            dma((5,)),
            dma((12,)), dma((12,)),
            dma((12,)), dma((12,)),
            dma((10,)), dma((10,)),
            dma((22,)), dma((22,)),
            dma((7,)), dma((7,)),
        ],
        compiler_params=pltpu.CompilerParams(
            collective_id=0, has_side_effects=True, vmem_limit_bytes=VMEM_BYTES
        ),
    )(*[pltpu.with_memory_space_constraint(x, pltpu.HBM) for x in operands])


def solution(mesh):
    return jax.shard_map(
        device_program,
        mesh=mesh,
        in_specs=(
            P(("parts", "cluster"), None),
            P(("parts", "cluster"), None, None),
            P(("parts", "cluster"), None),
            P(("parts", "cluster"), None),
        ),
        out_specs=(P(("parts", "cluster"), None), P(("parts", "cluster"), None, None)),
        check_vma=False,
    )
```

```python
import functools

import jax
import jax.numpy as jnp
from jax import lax
from jax.experimental import pallas as pl
from jax.experimental.pallas import tpu as pltpu
from jax.sharding import PartitionSpec as P

SOFTMAX_HEAT = 2.0
FEEDBACK = 0.5
MASKED = -1e30
VMEM_BYTES = 50 * 1024 * 1024


def position_targets(block_ids, capacity):
    flat_ids = block_ids.reshape(-1)
    matches = flat_ids[:, None] == flat_ids[None, :]
    positions = jnp.arange(flat_ids.shape[0], dtype=jnp.int32)
    earlier = positions[None, :] < positions[:, None]
    ranking = jnp.sum(jnp.logical_and(matches, earlier), axis=1, dtype=jnp.int32)
    return flat_ids * capacity + ranking


def pack_rows(values, targets, owners, resident_blocks, capacity):
    buffer = jnp.zeros((owners * resident_blocks * capacity, values.shape[1]), values.dtype)
    buffer = buffer.at[targets].set(values)
    return buffer.reshape(owners, resident_blocks, capacity, values.shape[1])


def reply(results):
    return (
        lax.all_to_all(results[0], "cluster", split_axis=0, concat_axis=0, tiled=True),
        lax.all_to_all(results[1], "cluster", split_axis=0, concat_axis=0, tiled=True),
        lax.all_to_all(results[2], "cluster", split_axis=0, concat_axis=0, tiled=True),
    )


def send_back(match_scores):
    return lax.all_to_all(match_scores, "cluster", split_axis=0, concat_axis=0, tiled=True)


def local(queries, passages, first_blocks, followup_blocks):
    owners = lax.axis_size("cluster")
    resident_blocks = passages.shape[0]
    embed_width = queries.shape[1]
    per_query = first_blocks.shape[1]
    pair_count = queries.shape[0] * per_query
    all_blocks = owners * resident_blocks
    capacity = max(2, (3 * pair_count + 2 * all_blocks - 1) // (2 * all_blocks))
    coefficient = FEEDBACK * embed_width ** (-0.5)
    highest = lax.Precision.HIGHEST

    def project_onto_centroid(arrived):
        return jnp.einsum("nbce,bre->nbcr", arrived, passages, precision=highest)

    first_targets = position_targets(first_blocks, capacity)
    second_targets = position_targets(followup_blocks, capacity)
    repeated = jnp.repeat(queries, per_query, axis=0)
    first_sent = pack_rows(repeated, first_targets, owners, resident_blocks, capacity)
    match_scores = SOFTMAX_HEAT * project_onto_centroid(
        lax.all_to_all(first_sent, "cluster", split_axis=0, concat_axis=0, tiled=True)
    )
    highs = jnp.max(match_scores, axis=3)
    weights = jnp.exp(match_scores - highs[..., None])
    totals = jnp.sum(weights, axis=3)
    vectors = jnp.einsum("nbcr,bre->nbce", weights, passages, precision=highest)
    highs, totals, vectors = reply((highs, totals, vectors))
    highs = highs.reshape(-1)[first_targets].reshape(-1, per_query)
    totals = totals.reshape(-1)[first_targets].reshape(-1, per_query)
    vectors = vectors.reshape(-1, embed_width)[first_targets].reshape(-1, per_query, embed_width)
    peak_high = jnp.max(highs, axis=1, keepdims=True)
    scaled = jnp.exp(highs - peak_high)
    denominator = jnp.sum(scaled * totals, axis=1)
    feedback = jnp.einsum("qk,qke->qe", scaled, vectors, precision=highest) / denominator[:, None]
    expanded = queries + coefficient * feedback
    expanded_sent = pack_rows(
        jnp.repeat(expanded, per_query, axis=0), second_targets, owners, resident_blocks, capacity
    )
    returned = (lambda arrived: send_back(project_onto_centroid(arrived)))(
        lax.all_to_all(expanded_sent, "cluster", split_axis=0, concat_axis=0, tiled=True)
    )
    second_scores = returned.reshape(-1, returned.shape[3])[second_targets].reshape(
        queries.shape[0], per_query, -1
    )
    return (expanded, second_scores)


def dot_nt(a, b):
    return lax.dot_general(a, b, (((1,), (1,)), ((), ())), preferred_element_type=jnp.float32)


def dot_nn(a, b):
    return lax.dot_general(a, b, (((1,), (0,)), ((), ())), preferred_element_type=jnp.float32)


def halves(x):
    high = x.astype(jnp.bfloat16)
    return high, (x - high.astype(jnp.float32)).astype(jnp.bfloat16)


def tools_of(
    corpus, turned_hi, turned_lo, pair, total, asked, chosen, picked, names_of, part
):
    both_rows = total.shape[0]
    top, _, size = asked.shape
    piece = size // 2
    lane = lax.broadcasted_iota(jnp.int32, (1, size), 1)

    def put_pair(x, offset=0):
        high, low = halves(x)
        pair[pl.ds(offset, x.shape[0]), :] = high
        pair[pl.ds(both_rows + offset, x.shape[0]), :] = low

    def spread_out(held, wide, g):
        rows = held.shape[2]
        for j in range(top):
            line = held[g, j : j + 1, :].astype(jnp.float32)
            wide[j, pl.ds(g * rows, rows), :] = jnp.broadcast_to(line, (size, rows)).T

    def absorb(pieces, count, carry, offset=0):
        peak, norm = carry
        group = pl.ds(offset, count)
        highs, lows, names = [], [], []
        for unit, h in pieces:
            high, low = turn_over(unit, unit, h)
            highs.append(high)
            lows.append(low)
            own, others = names_of(unit)
            names.append(jnp.where(lane < piece, own, others))
        wide = [
            jnp.concatenate([turned[unit, :, pl.ds(h * size, size)] for unit, h in pieces], axis=1)
            for turned in (turned_hi, turned_lo)
        ]
        all_found = dot_three(
            pair[group, :], pair[pl.ds(both_rows + offset, count), :], *wide
        )
        sums = [all_found[:, k * size : (k + 1) * size] for k in range(len(pieces))]
        parts, hits = [], []
        top_score = peak
        for name, found in zip(names, sums):
            hit = asked[0, group, :] == name
            for j in range(1, top):
                hit = jnp.logical_or(hit, asked[j, group, :] == name)
            score = jnp.where(hit, SOFTMAX_HEAT * found, MASKED)
            top_score = jnp.maximum(top_score, jnp.max(score, axis=1, keepdims=True))
            parts.append(score)
            hits.append(hit)
        shrink = jnp.exp(peak - top_score)
        weights = jnp.concatenate(
            [jnp.where(hit, jnp.exp(score - top_score), 0.0) for hit, score in zip(hits, parts)], axis=1
        )
        norm = norm * shrink + jnp.sum(weights, axis=1, keepdims=True)
        weight_high, weight_low = halves(weights)
        mixed = dot_three(
            weight_high, weight_low, jnp.concatenate(highs, axis=0), jnp.concatenate(lows, axis=0)
        )
        total[group, :] = total[group, :] * shrink + mixed
        return top_score, norm

    def turn_over(source, unit, h):
        high, low = halves(
            jnp.concatenate([corpus[source, 0, part(h), :], corpus[source, 1, part(h), :]], axis=0)
        )
        place = pl.ds(h * size, size)
        turned_hi[unit, :, place] = high.T
        turned_lo[unit, :, place] = low.T
        return high, low

    def score_units(g, rows, turns, starts, strides):
        group = pl.ds(g * rows, rows)

        def second_round(turn, carry):
            values = [picked[j, group, :] for j in range(top)]
            for start, stride in zip(starts, strides):
                unit = start + stride * turn
                found = dot_three(
                    pair[group, :], pair[pl.ds(both_rows + g * rows, rows), :],
                    turned_hi[unit], turned_lo[unit],
                )
                a, b = found[:, :size], found[:, size:]
                own = jnp.where(lane < piece, a, pltpu.roll(b, piece, 1))
                others = jnp.where(lane < piece, pltpu.roll(a, piece, 1), b)
                names = names_of(unit)
                for j in range(top):
                    value = jnp.where(chosen[j, group, :] == names[0], own, values[j])
                    values[j] = jnp.where(chosen[j, group, :] == names[1], others, value)
            for j in range(top):
                picked[j, group, :] = values[j]
            return carry

        lax.fori_loop(0, turns, second_round, 0)

    return put_pair, spread_out, absorb, turn_over, score_units


def dot_three(high, low, right_high, right_low):
    return dot_nn(high, right_high) + (dot_nn(low, right_high) + dot_nn(high, right_low))


def nothing_yet(count):
    return jnp.full((count, 1), MASKED, jnp.float32), jnp.zeros((count, 1), jnp.float32)


def hub_kernel(
    queries_in, passages, first_in, followup_in, expanded, scores,
    first, followup, corpus, turned_hi, turned_lo, queries, pair, total, asked, chosen, picked,
    early, stats, scores_out,
    load_sem, send_c, recv_c, send_y, recv_y, send_z, recv_z, send_x, recv_x, send_back, recv_back,
):
    me = lax.axis_index("cluster")
    core, y, z = me % 2, (me // 2) % 2, me // 4
    rows, width = expanded.shape
    both_rows = 2 * rows
    top, _, size = asked.shape
    piece = size // 2
    inner = ((z + 1) % 4) // 2
    mate_z = z + 1 - 2 * (z % 2)
    hub_z = inner * z + (1 - inner) * mate_z
    end_z = inner * mate_z + (1 - inner) * z
    far_hub, far_end = 3 - hub_z, 3 - end_z

    def device(zz, yy, cc):
        return (2 * zz + yy) * 2 + cc

    mate = device(mate_z, y, core)
    beside = device(z, 1 - y, core)
    far = device(3 - z, y, core)
    other = device(z, y, 1 - core)

    plan = (
        (hub_z, y, 0), (hub_z, y, 1),
        (end_z, y, 0), (end_z, y, 1), (end_z, 1 - y, 1), (end_z, 1 - y, 0),
        (hub_z, 1 - y, 0), (hub_z, 1 - y, 1), (far_hub, 1 - y, 0), (far_hub, 1 - y, 1), (far_end, 1 - y, 0),
        (far_hub, y, 0), (far_hub, y, 1), (far_end, y, 0), (far_end, y, 1), (far_end, 1 - y, 1),
    )

    def names_of(unit):
        chip, index = 0, 0
        for k, (zz, yy, ii) in enumerate(plan):
            here = jnp.int32(unit == k) if isinstance(unit, int) else (unit == k).astype(jnp.int32)
            chip = chip + here * (2 * zz + yy)
            index = index + here * ii
        return (
            ((2 * chip + core) * 2 + index).astype(jnp.float32),
            ((2 * chip + 1 - core) * 2 + index).astype(jnp.float32),
        )

    def remote(src, dst, send, recv, target):
        return pltpu.make_async_remote_copy(
            src_ref=src, dst_ref=dst, send_sem=send, recv_sem=recv,
            device_id={"cluster": target}, device_id_type=pl.DeviceIdType.MESH,
        )

    def part(h):
        return pl.ds(h * piece, piece)

    def unit_copy(source, unit, sems, k, target):
        return remote(corpus.at[source, 0], corpus.at[unit, 0], sems[0].at[k], sems[1].at[k], target)

    def half_copy(source, unit, h, sems, k, target):
        return remote(
            corpus.at[source, 0, part(h)], corpus.at[unit, 0, part(h)],
            sems[0].at[k], sems[1].at[k], target,
        )

    on_c, on_y, on_z, on_x = (send_c, recv_c), (send_y, recv_y), (send_z, recv_z), (send_x, recv_x)

    def ids_up(k):
        held = (first, followup)[k]
        return remote(held.at[0], held.at[1], send_c.at[k], recv_c.at[k], mate)

    def queries_up():
        return remote(
            queries.at[pl.ds(0, rows)], queries.at[pl.ds(rows, rows)], send_c.at[2], recv_c.at[2], mate
        )

    def up(unit, h):
        source = unit - 2 if isinstance(unit, int) and unit < 4 else unit
        return half_copy(source, unit, h, on_c, 2 * unit + h, mate)

    def side(unit):
        return unit_copy(unit - 3 if isinstance(unit, int) and unit > 7 else unit, unit, on_y, unit, beside)

    def across(unit):
        return remote(corpus.at[unit, 0], corpus.at[unit, 1], send_x.at[unit], recv_x.at[unit], other)

    def across_half(unit, h):
        k = 16 + (unit // 5 - 1) * 2 + h
        return remote(
            corpus.at[unit, 0, part(h)], corpus.at[unit, 1, part(h)], send_x.at[k], recv_x.at[k], other
        )

    def back(k):
        source, target = (
            (early.at[0], early.at[1]),
            (stats.at[0], stats.at[1]),
            (scores_out, scores),
        )[k]
        return remote(source, target, send_back.at[k], recv_back.at[k], mate)

    def down(unit, h):
        k = 3 + 2 * (unit - 13) + h
        return half_copy(unit, unit, h, (send_back, recv_back), k, mate)

    loads = (
        pltpu.make_async_copy(passages.at[0], corpus.at[0, 0], load_sem.at[0]),
        pltpu.make_async_copy(passages.at[1], corpus.at[1, 0], load_sem.at[1]),
        pltpu.make_async_copy(queries_in, queries.at[pl.ds(0, rows)], load_sem.at[2]),
        pltpu.make_async_copy(first_in, first.at[0], load_sem.at[3]),
        pltpu.make_async_copy(followup_in, followup.at[0], load_sem.at[4]),
    )
    for load in loads:
        load.start()
    barrier = pltpu.get_barrier_semaphore()
    for target in (mate, beside, other):
        pl.semaphore_signal(
            barrier, inc=1, device_id={"cluster": target}, device_id_type=pl.DeviceIdType.MESH
        )

    @pl.when(inner == 1)
    def _():
        pl.semaphore_signal(
            barrier, inc=1, device_id={"cluster": far}, device_id_type=pl.DeviceIdType.MESH
        )

    pl.semaphore_wait(barrier, 3 + inner)
    for load in loads:
        load.wait()

    @pl.when(inner == 0)
    def _():
        ids_up(0).start()
        ids_up(1).start()
        queries_up().start()
        corner_side = [
            remote(corpus.at[k, 0], corpus.at[5 - k, 0], send_y.at[k], recv_y.at[k], beside)
            for k in (1, 0)
        ]
        for copy in corner_side:
            copy.start()
        for unit in (2, 3):
            for h in range(2):
                up(unit, h).start()
        put_pair, spread_out, absorb, turn_over, score_units = tools_of(
            corpus, turned_hi, turned_lo, pair, total, asked, chosen, picked, names_of, part
        )
        put_pair(queries[pl.ds(0, rows), :])
        spread_out(first, asked, 0)
        spread_out(followup, chosen, 0)
        own = pl.ds(0, rows)
        for k in range(2):
            across(k).start()
        for j in range(top):
            picked[j, own, :] = jnp.zeros((rows, size), jnp.float32)
        total[own, :] = jnp.zeros((rows, width), jnp.float32)
        for copy, unit in zip(corner_side, (4, 5)):
            copy.wait_recv()
            for h in range(2):
                up(unit, h).start()
        for h in range(2):
            across_half(5, h).start()
        across(4).start()
        for source, unit in ((0, 2), (1, 3)):
            across(source).wait_recv()
            for h in range(2):
                turn_over(source, unit, h)
        across(4).wait_recv()
        carry = absorb([(4, 0), (4, 1)], rows, nothing_yet(rows))
        passed = [
            remote(
                corpus.at[source, 0, part(h)], corpus.at[unit, 0, part(h)],
                send_y.at[unit // 5 * 2 + h - 2], recv_y.at[unit // 5 * 2 + h - 2], beside,
            )
            for source, unit in ((13, 10), (14, 15))
            for h in range(2)
        ]

        def share(k):
            passed[k].wait_recv()
            across_half(10 + k // 2 * 5, k % 2).start()

        for k in range(4):
            down(13 + k // 2, k % 2).wait_recv()
            passed[k].start()
            if k % 2 == 1:
                across(13 + k // 2).start()
            if k > 0:
                share(k - 1)
            if k == 2:
                across(13).wait_recv()
        share(3)

        def late(h, carry):
            for unit in (5, 10, 15):
                across_half(unit, h).wait_recv()
            return absorb([(5, h), (10, h), (15, h)], rows, carry)

        for h in range(2):
            turn_over(13, 13, h)
        across(14).wait_recv()
        carry = absorb([(14, 0), (14, 1)], rows, carry)
        peak, norm = lax.fori_loop(0, 2, late, carry)
        for k in range(2):
            back(k).wait_recv()
        early_peak, early_norm = (
            jnp.broadcast_to(stats[1, k, 0:1, :], (size, rows)).T[:, 0:1] for k in range(2)
        )
        top_score = jnp.maximum(peak, early_peak)
        shrink, early_shrink = jnp.exp(peak - top_score), jnp.exp(early_peak - top_score)
        norm = norm * shrink + early_norm * early_shrink
        mixed = total[own, :] * shrink + early[1] * early_shrink
        after = queries[own, :] + (FEEDBACK * width ** (-0.5)) * (mixed / norm)
        expanded[...] = after
        put_pair(after)
        score_units(0, rows, 2, (2, 3, 4, 5), (8, 10, 10, 10))
        back(2).wait_recv()
        for j in range(top):
            scores[:, j, :] = scores[:, j, :] + picked[j, own, :]
        for unit in (0, 1, 4, 13, 14):
            across(unit).wait_send()
        for copy in passed:
            copy.wait_send()
        for unit in (5, 10, 15):
            for h in range(2):
                across_half(unit, h).wait_send()
        ids_up(0).wait_send()
        ids_up(1).wait_send()
        queries_up().wait_send()
        for copy in corner_side:
            copy.wait_send()
        for unit in (2, 3, 4, 5):
            for h in range(2):
                up(unit, h).wait_send()

    @pl.when(inner == 1)
    def _():
        hub(
            first, followup, corpus, turned_hi, turned_lo, queries, pair, total, asked, chosen,
            picked, expanded, scores, early, stats, scores_out,
            names_of, unit_copy, half_copy, ids_up, queries_up, across, across_half, back, down, part,
            on_c, on_y, on_z, mate, beside, far,
        )


def hub(
    first, followup, corpus, turned_hi, turned_lo, queries, pair, total, asked, chosen,
    picked, expanded, scores, early, stats, scores_out,
    names_of, unit_copy, half_copy, ids_up, queries_up, across, across_half, back, down, part,
    on_c, on_y, on_z, mate, beside, far,
):
    rows, width = expanded.shape
    both_rows = 2 * rows
    top, _, size = asked.shape
    piece = size // 2
    lane = lax.broadcasted_iota(jnp.int32, (1, size), 1)

    def from_mate(unit, h):
        return half_copy(unit, unit, h, on_c, 2 * unit + h, mate)

    def from_side(t):
        return unit_copy(5 + t, 5 + t, on_y, 5 + t, beside)

    def last_side(h):
        return half_copy(13, 10, h, on_y, 10 + h, beside)

    def own_side(k):
        return unit_copy(k, 6 + k, on_y, 6 + k, beside)

    def pass_side(t):
        return unit_copy(10 + t, 7 + t, on_y, 7 + t, beside)

    def own_far(k):
        return unit_copy(k, 11 + k, on_z, k, far)

    def pass_far(t, h):
        return half_copy(t, 11 + t, h, on_z, 2 * t + h, far)

    def from_far(t):
        return unit_copy(10 + t, 10 + t, on_z, t - 1, far)

    def from_far_half(t, h):
        return half_copy(10 + t, 10 + t, h, on_z, 2 * (t - 1) + h, far)

    for k in range(2):
        own_far(k).start()
        own_side(k).start()
    for k in range(2):
        across(k).start()
    from_far(1).wait_recv()
    pass_side(1).start()
    across(11).start()
    from_side(1).wait_recv()
    across(6).start()
    for k in range(2):
        ids_up(k).wait_recv()
    queries_up().wait_recv()

    put_pair, spread_out, absorb, turn_over, score_units = tools_of(
        corpus, turned_hi, turned_lo, pair, total, asked, chosen, picked, names_of, part
    )
    put_pair(queries[...])
    total[...] = jnp.zeros_like(total)
    picked[...] = jnp.zeros_like(picked)
    for g in range(2):
        spread_out(first, asked, g)
        spread_out(followup, chosen, g)

    def take(unit, carry):
        across(unit).wait_recv()
        return absorb([(unit, 0), (unit, 1)], both_rows, carry)

    def step(t, carry):
        carry = take(4 + t, carry)

        @pl.when(t == 5)
        def _():
            early[0] = total[pl.ds(rows, rows), :]
            for k in range(2):
                line = jnp.broadcast_to(carry[k][rows:], (rows, size)).T
                stats[0, k] = line[: stats.shape[2], :]
            back(1).start()
            back(0).start()

        carry = take(t - 1, carry)

        @pl.when(t < 5)
        def _():
            from_mate(t, 0).wait_recv()
            pass_far(t, 0).start()

            @pl.when(t > 2)
            def _():
                from_far_half(t, 0).wait_recv()
                down(10 + t, 0).start()

        carry = take(9 + t, carry)

        @pl.when(t < 5)
        def _():
            from_mate(t, 1).wait_recv()
            pass_far(t, 1).start()
            across(t).start()

            @pl.when(t == 2)
            def _():
                from_far(t).wait_recv()
                pass_side(t).start()

            @pl.when(t > 2)
            def _():
                from_far_half(t, 1).wait_recv()
                down(10 + t, 1).start()

            across(10 + t).start()
            from_side(t).wait_recv()
            across(5 + t).start()

            @pl.when(t == 3)
            def _():
                for h in range(2):
                    last_side(h).start()

        return carry

    carry = nothing_yet(both_rows)
    carry = take(0, carry)
    carry = lax.fori_loop(2, 6, step, carry)

    def arrive(h):
        from_mate(5, h).wait_recv()
        across_half(5, h).start()
        last_side(h).wait_recv()
        across_half(10, h).start()
        from_far_half(5, h).wait_recv()
        across_half(15, h).start()
        for unit in (5, 10, 15):
            across_half(unit, h).wait_recv()
        return [(5, h), (10, h), (15, h)]

    def expand(offset, norm):
        group = pl.ds(offset, rows)
        return queries[group, :] + (FEEDBACK * width ** (-0.5)) * (total[group, :] / norm)

    carry = absorb(arrive(0), both_rows, carry)
    _, norm = absorb(arrive(1), rows, (carry[0][rows:], carry[1][rows:]), rows)
    put_pair(expand(rows, norm), rows)
    score_units(1, rows, 2, (0, 1, 6, 7), (8, 8, 5, 5))
    for j in range(top):
        scores_out[:, j, :] = picked[j, pl.ds(rows, rows), :]
    back(2).start()
    _, norm = absorb(
        [(unit, 1) for unit in (5, 10, 15)], rows, (carry[0][:rows], carry[1][:rows])
    )
    after = expand(0, norm)
    put_pair(after)
    expanded[...] = after
    score_units(0, rows, 4, (0, 1, 2, 3), (4, 4, 4, 4))
    for j in range(top):
        scores[:, j, :] = picked[j, pl.ds(0, rows), :]

    for k in range(2):
        own_far(k).wait_send()
        own_side(k).wait_send()
        pass_side(1 + k).wait_send()
        last_side(k).wait_send()
    for k in range(3):
        back(k).wait_send()
    for unit in (13, 14):
        for h in range(2):
            down(unit, h).wait_send()

    def drain(t, carry):
        for h in range(2):
            pass_far(t, h).wait_send()
        return carry

    lax.fori_loop(2, 5, drain, 0)

    def drain_across(unit, carry):
        @pl.when(unit % 5 != 0)
        def _():
            across(unit).wait_send()

        return carry

    across(0).wait_send()
    lax.fori_loop(1, 15, drain_across, 0)
    for unit in (5, 10, 15):
        for h in range(2):
            across_half(unit, h).wait_send()


def grant_of(queries, passages, first_blocks):
    resident, size, width = passages.shape
    rows = queries.shape[0]
    corpus = lax.axis_size("cluster") * resident * size * width * 8
    return corpus + (12 * rows * width + 10 * first_blocks.shape[1] * rows * size) * 4


def hub_fits(queries, passages, first_blocks):
    owners = lax.axis_size("cluster")
    resident, size, _ = passages.shape
    fits = grant_of(queries, passages, first_blocks) < VMEM_BYTES
    return owners == 16 and resident == 2 and fits and queries.shape[0] == size


def device_program(queries, passages, first_blocks, followup_blocks):
    if not hub_fits(queries, passages, first_blocks):
        return local(queries, passages, first_blocks, followup_blocks)
    units = lax.axis_size("cluster")
    rows, width = queries.shape
    size = passages.shape[1]
    top = first_blocks.shape[1]
    vmem = pl.BlockSpec(memory_space=pltpu.VMEM)
    hbm = pl.BlockSpec(memory_space=pltpu.HBM)
    operands = (queries, passages, first_blocks.T, followup_blocks.T)
    dma = pltpu.SemaphoreType.DMA
    return pl.pallas_call(
        hub_kernel,
        out_shape=(
            jax.ShapeDtypeStruct((rows, width), jnp.float32),
            jax.ShapeDtypeStruct((rows, top, size), jnp.float32),
        ),
        in_specs=[hbm, hbm, hbm, hbm],
        out_specs=(vmem, vmem),
        scratch_shapes=[
            pltpu.VMEM((2, top, rows), jnp.int32),
            pltpu.VMEM((2, top, rows), jnp.int32),
            pltpu.VMEM((units, 2, size, width), jnp.float32),
            pltpu.VMEM((units, width, 2 * size), jnp.bfloat16),
            pltpu.VMEM((units, width, 2 * size), jnp.bfloat16),
            pltpu.VMEM((2 * rows, width), jnp.float32),
            pltpu.VMEM((4 * rows, width), jnp.bfloat16),
            pltpu.VMEM((2 * rows, width), jnp.float32),
            pltpu.VMEM((top, 2 * rows, size), jnp.float32),
            pltpu.VMEM((top, 2 * rows, size), jnp.float32),
            pltpu.VMEM((top, 2 * rows, size), jnp.float32),
            pltpu.VMEM((2, rows, width), jnp.float32),
            pltpu.VMEM((2, 2, 8, rows), jnp.float32),
            pltpu.VMEM((rows, top, size), jnp.float32),
            dma((5,)),
            dma((12,)), dma((12,)),
            dma((12,)), dma((12,)),
            dma((10,)), dma((10,)),
            dma((22,)), dma((22,)),
            dma((7,)), dma((7,)),
        ],
        compiler_params=pltpu.CompilerParams(
            collective_id=0, has_side_effects=True, vmem_limit_bytes=VMEM_BYTES
        ),
    )(*[pltpu.with_memory_space_constraint(x, pltpu.HBM) for x in operands])


def solution(mesh):
    return jax.shard_map(
        device_program,
        mesh=mesh,
        in_specs=(
            P(("parts", "cluster"), None),
            P(("parts", "cluster"), None, None),
            P(("parts", "cluster"), None),
            P(("parts", "cluster"), None),
        ),
        out_specs=(P(("parts", "cluster"), None), P(("parts", "cluster"), None, None)),
        check_vma=False,
    )
```
